128 devices in a mesh: dp: 8 (over x, core), vocab: 16 (over y, z).
Axes of the slice: x: 4, y: 4, z: 4, core: 2. Of those that a mesh axis runs over, the one named last changes fastest.
Arguments:
- hidden: bfloat16 [512, 3584], P('dp'), may hold values from -160 to 160
- head_weight: bfloat16 [3584, 152064], P(None, ('dp', 'vocab')), may hold values from -0.3125 to 0.3125
- teacher_ids: int32 [512, 64], P('dp'), may hold values from 0 to 152063, as said below
- teacher_probs: float32 [512, 64], P('dp'), may hold values from 0 to 0.99, as said below
- token_weight: float32 [512], P('dp'), may hold values from 4 to 32
Outputs:
- divergence: float32 [512], P('dp')
- hidden_grad: float32 [512, 3584], P('dp', 'vocab')
The draws below stay inside these ranges and needn't reach their ends.
Inputs may be any that keep to these rules, and one draw needn't show every extreme that they name: `teacher_ids`: each row names 64 different vocabulary entries. `teacher_probs`: all positive; each row sums to between 0.5 and 0.99.
All inputs are finite; a program needn't handle non-finite values.
Results may differ from the reference program's by a relative error of at most 0.0029.
Values may be sent and summed in bfloat16 or wider, within the bound.
A program may use at most 128 MiB of HBM per device.

```python
import math
import jax
import jax.numpy as jnp
from jax import lax

D = 3584
V = 152064
TOP = 64
TOKENS = 512


def draw_hidden(key, part):
    base = jnp.clip(jax.random.normal(key, (TOKENS, D), jnp.float32), -4.0, 4.0)
    return base.astype(jnp.bfloat16)


def draw_teacher_ids(key, part):
    spread = jax.random.randint(key, (TOKENS, TOP), 0, V - TOP + 1, dtype=jnp.int32)
    ordered = jnp.sort(spread, axis=1) + jnp.arange(TOP, dtype=jnp.int32)[None, :]
    order_keys = jax.random.randint(jax.random.fold_in(key, 1), (TOKENS, TOP), 0, 1 << 20, dtype=jnp.int32) * TOP + jnp.arange(TOP, dtype=jnp.int32)[None, :]
    shuffle = jnp.argsort(order_keys, axis=1)
    return jnp.take_along_axis(ordered, shuffle, axis=1).astype(jnp.int32)


def draw_teacher_probs(key, part):
    raw = jnp.exp(jnp.clip(1.5 * jax.random.normal(key, (TOKENS, TOP), jnp.float32), -4.5, 4.5))
    totals = jax.random.uniform(jax.random.fold_in(key, 2), (TOKENS, 1), jnp.float32, 0.5, 0.99)
    return (totals * raw / jnp.sum(raw, axis=1, keepdims=True)).astype(jnp.float32)


def shard_levels(own_key, extent, cuts, low, top_value):
    gain, own = 1.0, jax.random.fold_in(own_key, 6)
    for position, parts in cuts:
        heights = jnp.exp(jax.random.uniform(jax.random.fold_in(own, position), (parts,), jnp.float32, low / len(cuts), top_value / len(cuts)))
        gain = gain * jnp.repeat(heights, extent[position] // parts).reshape([-1 if axis == position else 1 for axis in range(len(extent))])
    return gain


def centred(own_key, shape, scale, most, shards=(), kind=jnp.bfloat16):
    values = jax.random.normal(own_key, shape, jnp.float32) * scale
    if len(shards) > 0:
        values = shard_levels(own_key, shape, shards, -0.22, 0.18) * values
    return jnp.clip(values, min=-most, max=most).astype(kind)


def setup_inputs(seed: int = 0) -> dict:
    keys = jax.random.split(jax.random.key(seed), 6)
    hidden = draw_hidden(jax.random.fold_in(keys[5], 71), 0)
    head_weight = centred(keys[1], (D, V), (D // 9) ** -0.5, 0.3125, ((1, 128),))
    teacher_ids = draw_teacher_ids(jax.random.fold_in(keys[5], 71), 0)
    teacher_probs = draw_teacher_probs(jax.random.fold_in(keys[5], 71), 0)
    token_weight = jnp.clip(jnp.exp(math.log(32.0) - 2.0794415 * jax.random.uniform(keys[4], (TOKENS,), jnp.float32) ** shard_levels(keys[4], (TOKENS,), ((0, 8),), -0.2, 0.2)), 4.0, 32.0)
    return {"hidden": hidden, "head_weight": head_weight, "teacher_ids": teacher_ids, "teacher_probs": teacher_probs, "token_weight": token_weight}


def reference(hidden, head_weight, teacher_ids, teacher_probs, token_weight):
    block = math.gcd(TOKENS, 128)
    count = TOKENS // block

    def one_block(index):
        first = index * block
        rows_in = lax.dynamic_slice_in_dim(hidden, first, block, 0)
        chosen = lax.dynamic_slice_in_dim(teacher_ids, first, block, 0)
        probs = lax.dynamic_slice_in_dim(teacher_probs, first, block, 0)
        weights = lax.dynamic_slice_in_dim(token_weight, first, block, 0)
        logits = jnp.dot(rows_in, head_weight, preferred_element_type=jnp.float32)
        largest = jnp.max(logits, axis=1)
        expsum = jnp.sum(jnp.exp(logits - largest[:, None]), axis=1)
        log_norm = largest + jnp.log(expsum)
        picked = jnp.take_along_axis(logits, chosen, axis=1)
        mass = jnp.sum(probs, axis=1)
        divergence = jnp.sum(probs * (jnp.log(probs) - picked + log_norm[:, None]), axis=1)
        sparse = jnp.zeros(logits.shape, jnp.float32).at[jnp.arange(block)[:, None], chosen].add(probs)
        logit_grad = (mass[:, None] * jnp.exp(logits - log_norm[:, None]) - sparse).astype(jnp.bfloat16)
        backward = lax.dot_general(logit_grad, head_weight, (((1,), (1,)), ((), ())), preferred_element_type=jnp.float32)
        return divergence, weights[:, None] * backward

    divergence, hidden_grad = lax.map(one_block, jnp.arange(count, dtype=jnp.int32))
    return divergence.reshape(TOKENS), hidden_grad.reshape(TOKENS, D)
```

```python
import functools

import jax
import jax.numpy as jnp
from jax import lax
from jax.experimental import pallas as pl
from jax.experimental.pallas import tpu as pltpu
from jax.sharding import Mesh
from jax.sharding import PartitionSpec as P

MESH = pl.DeviceIdType.MESH
DP = ("x", "c")
VOCAB = ("y", "z")
F32 = jnp.float32
BF16 = jnp.bfloat16
COLOURS = (
    (("x", "y", "z"), ((0, 16), (0, 8))),
    (("y", "z", "x"), ((16, 8), (8, 16))),
    (("z", "x", "y"), ((24, 8), (24, 8))),
)
WIRE2 = F32


def kernel(h, w, ids, pr, tw, out, dv, *scratch, names):
    S = dict(zip(names, scratch))
    D = h.shape[1]
    C = w.shape[1]
    TOP = ids.shape[1]
    Z = D // 16
    co = {a: lax.axis_index(a) for a in ("x", "c", "y", "z")}
    x, c, y, z = co["x"], co["c"], co["y"], co["z"]
    oc = 1 - c
    count = [0]

    def step(axis, d):
        return lax.rem(co[axis] + d, 4)

    def send(src, dst, **dev):
        i = count[0]
        count[0] += 1
        cp = pltpu.make_async_remote_copy(
            src_ref=src, dst_ref=dst, send_sem=S["ss"].at[i], recv_sem=S["rs"].at[i],
            device_id=dev, device_id_type=MESH,
        )
        cp.start()
        sent.append(cp)
        return cp

    sent = []
    wcopy = pltpu.make_async_copy(w, S["W"], S["ws"])
    wcopy.start()
    H, IP, W = S["H"], S["IP"], S["W"]
    me = c * 4 + x
    IP[me, :, 0:TOP] = pr[...]
    IP[me, :, TOP : 2 * TOP] = ids[...].astype(F32)
    for r in range(2):
        H[r, pl.ds(pl.multiple_of(me * 32, 32), 32), :] = h[r * 32 : r * 32 + 32, :]

    bar = pltpu.get_barrier_semaphore()
    for d in range(4):
        for e in range(2):
            if d or e:
                pl.semaphore_signal(
                    bar, inc=1, device_id={"x": step("x", d), "c": lax.rem(c + e, 2)}, device_id_type=MESH
                )
    for d in range(4):
        for e in range(4):
            if d or e:
                pl.semaphore_signal(
                    bar, inc=1, device_id={"y": step("y", d), "z": step("z", e)}, device_id_type=MESH
                )
    pl.semaphore_wait(bar, 22)

    share = (lax.rem(y + 2 * z, 4), lax.rem(2 * y + z, 4))
    X, Pn, Cn, In, Ic = [{}, {}], [{}, {}], [{}, {}], {}, {}

    def hrows(r, core, xb, off, n):
        return H.at[r, pl.ds(pl.multiple_of(core * 128 + xb * 32 + off, 8), n), :]

    def send_x(r):
        for d in (1, 3, 2):
            src = h.at[pl.ds(pl.multiple_of(r * 32 + share[r] * 8, 8), 8), :]
            X[r][d] = send(src, hrows(r, c, x, share[r] * 8, 8), x=step("x", d))
        Cn[r][0] = send(h.at[pl.ds(r * 32, 32), :], hrows(r, c, x, 0, 32), c=oc)

    def forward(r):
        full, half = (("y", "z"), ("z", "y"))[r]
        for d in (1, 3, 2):
            X[r][d].wait_recv()
            xs = step("x", 4 - d)
            rows = pl.ds(pl.multiple_of(c * 128 + xs * 32 + share[r] * 8, 8), 8)
            whole = H.at[r, rows, :]
            lo, hi = H.at[r, rows, 0 : D // 2], H.at[r, rows, D // 2 : D]
            Pn[r][d] = [
                send(whole, whole, **{full: step(full, 1)}),
                send(whole, whole, **{full: step(full, 3)}),
                send(lo, lo, **{half: step(half, 1)}),
                send(hi, hi, **{half: step(half, 3)}),
            ]

    def to_sibling(r):
        for d in (1, 3, 2):
            for cp in Pn[r][d]:
                cp.wait_recv()
            xs = step("x", 4 - d)
            blk = hrows(r, c, xs, 0, 32)
            Cn[r][d] = send(blk, blk, c=oc)

    send_x(0)
    for d in (1, 3, 2):
        In[d] = send(IP.at[me], IP.at[me], x=step("x", d))
    Ic[0] = send(IP.at[me], IP.at[me], c=oc)
    send_x(1)
    forward(0)
    for d in (1, 3, 2):
        In[d].wait_recv()
        s = c * 4 + step("x", 4 - d)
        Ic[d] = send(IP.at[s], IP.at[s], c=oc)
    forward(1)
    to_sibling(0)
    for d in range(4):
        Ic[d].wait_recv()

    dp_index = x * 2 + c
    offset = (dp_index * 16 + y * 4 + z) * C
    SP = S["SP"]

    def sparse(r, lo, hi):
        def group(g, _):
            blk = g // 2
            j0 = r * 32 + (g % 2) * 16
            rows = pl.ds(pl.multiple_of(j0, 16), 16)
            local = IP[blk, rows, TOP : 2 * TOP].astype(jnp.int32) - offset
            local = jnp.where((local >= 0) & (local < C), local, -1).astype(jnp.int16)
            lane = lax.broadcasted_iota(jnp.int32, (16, 128), 1)
            n = -(-C // 128)
            cols = [(lane + 128 * k).astype(jnp.int16) for k in range(n)]
            acc = [jnp.full((16, 128), 127, jnp.int16) for _ in range(n)]
            for k in range(TOP):
                one = jnp.broadcast_to(local[:, k : k + 1], (16, 128))
                for j in range(n):
                    acc[j] = jnp.where(one == cols[j], jnp.int16(k), acc[j])
            for j in range(n):
                which = acc[j].astype(jnp.int32)
                wide = min(128, C - 128 * j)
                for s in range(2):
                    table = IP[blk, pl.ds(pl.multiple_of(j0 + s * 8, 8), 8), :]
                    sel = which[s * 8 : s * 8 + 8]
                    got = jnp.where(sel < TOP, jnp.take_along_axis(table, sel, axis=1), 0.0)
                    SP[r, pl.ds(pl.multiple_of(g * 16 + s * 8, 8), 8), 128 * j : 128 * j + wide] = got[:, :wide]
            return 0

        lax.fori_loop(lo, hi, group, 0)

    eye = (
        lax.broadcasted_iota(jnp.int32, (128, 128), 0) == lax.broadcasted_iota(jnp.int32, (128, 128), 1)
    )

    def to_row(col):
        return jnp.sum(jnp.where(eye, jnp.broadcast_to(col, (128, 128)), 0.0), axis=0, keepdims=True)

    def to_col(row):
        return jnp.sum(jnp.where(eye, jnp.broadcast_to(row, (128, 128)), 0.0), axis=1, keepdims=True)

    L, ST = S["L"], S["ST"]
    SA, SB = S["SA"], S["SB"]

    def spread(buf, r, slot, near):
        ref = buf.at[r, slot]
        if near:
            return [
                send(ref, ref, x=step("x", d), c=lax.rem(c + e, 2))
                for d in range(4) for e in range(2) if d or e
            ]
        return [
            send(ref, ref, y=step("y", d), z=step("z", e))
            for d in range(4) for e in range(4) if d or e
        ]

    def first_dot(r):
        L[r] = jnp.dot(H[r], W[...], preferred_element_type=F32)

    def stats(r):
        def part(i, _):
            rows = pl.ds(pl.multiple_of(i * 32, 32), 32)
            v = L[r, rows, :]
            m = jnp.max(v, axis=1, keepdims=True)
            ST[rows, 0:1] = m
            ST[rows, 1:2] = jnp.sum(jnp.exp(v - m), axis=1, keepdims=True)
            return 0

        lax.fori_loop(0, 8, part, 0)
        for b in range(2):
            SA[r, me, b : b + 1, :] = to_row(ST[b * 128 : b * 128 + 128, 0:1])
            SA[r, me, b + 2 : b + 3, :] = to_row(ST[b * 128 : b * 128 + 128, 1:2])
        return spread(SA, r, me, True)

    def merged(buf, r, n, copies):
        for cp in copies:
            cp.wait_recv()
        m = buf[r, 0, 0:2, :]
        for k in range(1, n):
            m = jnp.maximum(m, buf[r, k, 0:2, :])
        s = jnp.zeros_like(m)
        for k in range(n):
            s = s + buf[r, k, 2:4, :] * jnp.exp(buf[r, k, 0:2, :] - m)
        return m, s

    plane = y * 4 + z

    def second_stats(r, copies):
        m, s = merged(SA, r, 8, copies)
        SB[r, plane, 0:2, :] = m
        SB[r, plane, 2:4, :] = s
        return spread(SB, r, plane, False)

    G, PK, LN = S["G"], S["PK"], S["LN"]

    def grads(r, copies):
        m, s = merged(SB, r, 16, copies)
        norm = m + jnp.log(s)
        for b in range(2):
            LN[r, b * 128 : b * 128 + 128, :] = to_col(norm[b : b + 1, :])

        def part(i, _):
            rows = pl.ds(pl.multiple_of(i * 32, 32), 32)
            v = L[r, rows, :]
            sp = SP[r, rows, :]
            mass = jnp.sum(IP[i, r * 32 : r * 32 + 32, 0:TOP], axis=1, keepdims=True)
            G[r, rows, :] = (mass * jnp.exp(v - LN[r, rows, :]) - sp).astype(BF16)
            PK[rows, :] = jnp.sum(sp * v, axis=1, keepdims=True)
            return 0

        lax.fori_loop(0, 8, part, 0)
        for b in range(2):
            S["QA"][r, me, b : b + 1, :] = to_row(PK[b * 128 : b * 128 + 128, :])

    PR, DS, DR = S["PR"], S["DS"], S["DR"]

    def second_dot(r, half):
        f0 = half * (D // 2)
        v = lax.dot_general(
            G[r], W[f0 : f0 + D // 2, :], (((1,), (1,)), ((), ())), preferred_element_type=F32
        )
        for i in range(8):
            PR[r, half * 8 + i] = v[:, i * Z : i * Z + Z]

        def cast(i, _):
            DS[r, half * 8 + i] = PR[r, half * 8 + i, pl.ds(pl.multiple_of(oc * 128, 128), 128), :].astype(BF16)
            return 0

        lax.fori_loop(0, 8, cast, 0)
        part = pl.ds(half * 8, 8)
        return send(DS.at[r, part], DR.at[r, part], c=oc)

    def place(order, yg, zg, xb):
        of = {"x": xb, "y": yg, "z": zg}
        return tuple(of[a] for a in order)

    def phase1(r, copies):
        for cp in copies:
            cp.wait_recv()

        def part(i, _):
            yg, zg = i // 4, i % 4
            for xb in range(4):
                mine = pl.ds(pl.multiple_of(c * 128 + xb * 32, 32), 32)
                v = PR[r, i, mine, :] + DR[r, i, xb * 32 : xb * 32 + 32, :].astype(F32)
                PR[r, i, mine, :] = v
                for k, (order, rows) in enumerate(COLOURS):
                    p, q, s = place(order, yg, zg, xb)
                    r0, n = rows[r]
                    S[f"T1{r}{k}"][p, q * 4 + s] = v[r0 : r0 + n].astype(BF16)
            return 0

        lax.fori_loop(0, 16, part, 0)
        res = []
        for k, (order, _) in enumerate(COLOURS):
            a = order[0]
            T, R = S[f"T1{r}{k}"], S[f"R1{r}{k}"]
            res.append([send(T.at[step(a, d)], R.at[d - 1], **{a: step(a, d)}) for d in (1, 3, 2)])
        return res

    def phase2(r, copies):
        res = []
        for k, (order, rows) in enumerate(COLOURS):
            for cp in copies[k]:
                cp.wait_recv()
            a, b, _ = order
            r0, n = rows[r]
            R, T = S[f"R1{r}{k}"], S[f"T2{r}{k}"]

            def part(i, _, order=order, r0=r0, n=n, R=R, T=T):
                at = dict(zip(order, (co[order[0]], i // 4, i % 4)))
                row = pl.ds(pl.multiple_of(c * 128 + at["x"] * 32 + r0, 8), n)
                v = PR[r, at["y"] * 4 + at["z"], row, :]
                for d in range(3):
                    v = v + R[d, i].astype(F32)
                T[i // 4, i % 4] = v.astype(T.dtype)
                return 0

            lax.fori_loop(0, 16, part, 0)
            R2 = S[f"R2{r}{k}"]
            res.append([send(T.at[step(b, d)], R2.at[d - 1], **{b: step(b, d)}) for d in (1, 3, 2)])
        return res

    def phase3(r, copies):
        res = []
        for k, (order, rows) in enumerate(COLOURS):
            for cp in copies[k]:
                cp.wait_recv()
            _, b, e = order
            T2, R2, T3, R3 = S[f"T2{r}{k}"], S[f"R2{r}{k}"], S[f"T3{r}{k}"], S[f"R3{r}{k}"]
            for s in range(4):
                v = T2[co[b], s].astype(F32)
                for d in range(3):
                    v = v + R2[d, s].astype(F32)
                T3[s] = v
            res.append([send(T3.at[step(e, d)], R3.at[d - 1], **{e: step(e, d)}) for d in (1, 3, 2)])
        return res

    def finish(r, copies, weight):
        for k, (order, rows) in enumerate(COLOURS):
            for cp in copies[k]:
                cp.wait_recv()
            r0, n = rows[r]
            T3, R3 = S[f"T3{r}{k}"], S[f"R3{r}{k}"]
            v = T3[co[order[2]]]
            for d in range(3):
                v = v + R3[d]
            lo = r * 32 + r0
            out[lo : lo + n, :] = weight[lo : lo + n, :] * v

    QA, QB = S["QA"], S["QB"]

    sparse(0, 0, 8)
    to_sibling(1)
    sparse(0, 8, 16)
    wcopy.wait()
    for d in range(4):
        Cn[0][d].wait_recv()
    first_dot(0)
    a0 = stats(0)
    for d in range(4):
        Cn[1][d].wait_recv()
    first_dot(1)
    b0 = second_stats(0, a0)
    a1 = stats(1)
    sparse(1, 0, 16)
    b1 = second_stats(1, a1)
    grads(0, b0)
    d0 = [second_dot(0, 0), second_dot(0, 1)]
    grads(1, b1)
    p0 = phase1(0, d0)
    d1 = [second_dot(1, 0), second_dot(1, 1)]
    qa = spread(QA, 0, me, True) + spread(QA, 1, me, True)
    p1 = phase1(1, d1)
    p0 = phase2(0, p0)
    for cp in qa:
        cp.wait_recv()
    for r in range(2):
        tot = QA[r, 0]
        for k in range(1, 8):
            tot = tot + QA[r, k]
        QB[r, plane] = tot
    qb = spread(QB, 0, plane, False) + spread(QB, 1, plane, False)
    p1 = phase2(1, p1)
    p0 = phase3(0, p0)
    p1 = phase3(1, p1)

    small = (
        lax.broadcasted_iota(jnp.int32, (64, 64), 0) == lax.broadcasted_iota(jnp.int32, (64, 64), 1)
    )
    weight = jnp.sum(jnp.where(small, jnp.broadcast_to(tw[...], (64, 64)), 0.0), axis=1, keepdims=True)
    for cp in qb:
        cp.wait_recv()
    for r in range(2):
        tot = QB[r, 0]
        for k in range(1, 16):
            tot = tot + QB[r, k]
        for b in range(2):
            PK[b * 128 : b * 128 + 128, :] = to_col(tot[b : b + 1, :])
        mine = pl.ds(pl.multiple_of(me * 32, 32), 32)
        q = pr[r * 32 : r * 32 + 32, :]
        mass = jnp.sum(q, axis=1, keepdims=True)
        S["DV"][r * 32 : r * 32 + 32, :] = (
            jnp.sum(q * jnp.log(q), axis=1, keepdims=True) - PK[mine, :] + mass * LN[r, mine, :]
        )
    dv[...] = jnp.sum(jnp.where(small, jnp.broadcast_to(S["DV"][...], (64, 64)), 0.0), axis=0, keepdims=True)
    finish(0, p0, weight)
    finish(1, p1, weight)
    for cp in sent:
        cp.wait_send()


def body(hidden, head_weight, teacher_ids, teacher_probs, token_weight):
    T, D = hidden.shape
    C = head_weight.shape[1]
    Z = D // 16
    V = pltpu.VMEM
    scratch = {
        "W": V((D, C), BF16), "H": V((2, 256, D), BF16), "IP": V((8, T, 128), F32),
        "SP": V((2, 256, C), F32), "L": V((2, 256, C), F32), "ST": V((256, 2), F32),
        "SA": V((2, 8, 8, 128), F32), "SB": V((2, 16, 8, 128), F32),
        "QA": V((2, 8, 8, 128), F32), "QB": V((2, 16, 8, 128), F32),
        "G": V((2, 256, C), BF16), "PK": V((256, 1), F32), "LN": V((2, 256, 1), F32),
        "DV": V((T, 1), F32),
        "PR": V((2, 16, 256, Z), F32), "DS": V((2, 16, 128, Z), BF16), "DR": V((2, 16, 128, Z), BF16),
    }
    for r in range(2):
        for k, (_, rows) in enumerate(COLOURS):
            n = rows[r][1]
            scratch[f"T1{r}{k}"] = V((4, 16, n, Z), BF16)
            scratch[f"R1{r}{k}"] = V((3, 16, n, Z), BF16)
            scratch[f"T2{r}{k}"] = V((4, 4, n, Z), WIRE2)
            scratch[f"R2{r}{k}"] = V((3, 4, n, Z), WIRE2)
            scratch[f"T3{r}{k}"] = V((4, n, Z), F32)
            scratch[f"R3{r}{k}"] = V((3, n, Z), F32)
    scratch["ss"] = pltpu.SemaphoreType.DMA((220,))
    scratch["rs"] = pltpu.SemaphoreType.DMA((220,))
    scratch["ws"] = pltpu.SemaphoreType.DMA
    vm = pl.BlockSpec(memory_space=pltpu.VMEM)
    grad, div = pl.pallas_call(
        functools.partial(kernel, names=tuple(scratch)),
        out_shape=(jax.ShapeDtypeStruct((T, Z), F32), jax.ShapeDtypeStruct((1, T), F32)),
        in_specs=[vm, pl.BlockSpec(memory_space=pl.ANY), vm, vm, vm],
        out_specs=(vm, vm),
        scratch_shapes=list(scratch.values()),
        compiler_params=pltpu.CompilerParams(
            collective_id=0, has_side_effects=True, vmem_limit_bytes=67043328
        ),
        name="distill",
    )(hidden, head_weight, teacher_ids, teacher_probs, token_weight.reshape(1, T))
    return div.reshape(T), grad


def solution(mesh):
    split = Mesh(mesh.devices.reshape(4, 2, 4, 4), ("x", "c", "y", "z"))
    placed = (P(DP, None), P(None, DP + VOCAB), P(DP, None), P(DP, None), P(DP))
    return jax.shard_map(
        body, mesh=split, in_specs=placed, out_specs=(P(DP), P(DP, VOCAB)), check_vma=False
    )
```

```python
import functools

import jax
import jax.numpy as jnp
from jax import lax
from jax.experimental import pallas as pl
from jax.experimental.pallas import tpu as pltpu
from jax.sharding import Mesh
from jax.sharding import PartitionSpec as P

MESH = pl.DeviceIdType.MESH
DP = ("x", "c")
VOCAB = ("y", "z")
F32 = jnp.float32
BF16 = jnp.bfloat16
COLOURS = (
    (("x", "y", "z"), ((0, 16), (0, 8))),
    (("y", "z", "x"), ((16, 8), (8, 16))),
    (("z", "x", "y"), ((24, 8), (24, 8))),
)
WIRE2 = F32


def kernel(h, w, ids, pr, tw, out, dv, *scratch, names):
    S = dict(zip(names, scratch))
    D = h.shape[1]
    C = w.shape[0]
    TOP = ids.shape[1]
    Z = D // 16
    co = {a: lax.axis_index(a) for a in ("x", "c", "y", "z")}
    x, c, y, z = co["x"], co["c"], co["y"], co["z"]
    oc = 1 - c
    count = [0]

    def step(axis, d):
        return lax.rem(co[axis] + d, 4)

    def send(src, dst, **dev):
        i = count[0]
        count[0] += 1
        cp = pltpu.make_async_remote_copy(
            src_ref=src, dst_ref=dst, send_sem=S["ss"].at[i], recv_sem=S["rs"].at[i],
            device_id=dev, device_id_type=MESH,
        )
        cp.start()
        sent.append(cp)
        return cp

    sent = []
    wcopy = pltpu.make_async_copy(w, S["W"], S["ws"])
    wcopy.start()
    H, IP, W = S["H"], S["IP"], S["W"]
    me = c * 4 + x
    IP[me, :, 0:TOP] = pr[...]
    IP[me, :, TOP : 2 * TOP] = ids[...].astype(F32)
    for r in range(2):
        H[r, pl.ds(pl.multiple_of(me * 32, 32), 32), :] = h[r * 32 : r * 32 + 32, :]

    bar = pltpu.get_barrier_semaphore()
    for d in range(4):
        for e in range(2):
            if d or e:
                pl.semaphore_signal(
                    bar, inc=1, device_id={"x": step("x", d), "c": lax.rem(c + e, 2)}, device_id_type=MESH
                )
    for d in range(4):
        for e in range(4):
            if d or e:
                pl.semaphore_signal(
                    bar, inc=1, device_id={"y": step("y", d), "z": step("z", e)}, device_id_type=MESH
                )
    pl.semaphore_wait(bar, 22)

    share = (lax.rem(y + 2 * z, 4), lax.rem(2 * y + z, 4))
    X, Pn, Cn, In, Ic = [{}, {}], [{}, {}], [{}, {}], {}, {}

    def hrows(r, core, xb, off, n):
        return H.at[r, pl.ds(pl.multiple_of(core * 128 + xb * 32 + off, 8), n), :]

    def send_x(r):
        for d in (1, 3, 2):
            src = h.at[pl.ds(pl.multiple_of(r * 32 + share[r] * 8, 8), 8), :]
            X[r][d] = send(src, hrows(r, c, x, share[r] * 8, 8), x=step("x", d))
        Cn[r][0] = send(h.at[pl.ds(r * 32, 32), :], hrows(r, c, x, 0, 32), c=oc)

    def forward(r):
        full, half = (("y", "z"), ("z", "y"))[r]
        for d in (1, 3, 2):
            X[r][d].wait_recv()
            xs = step("x", 4 - d)
            rows = pl.ds(pl.multiple_of(c * 128 + xs * 32 + share[r] * 8, 8), 8)
            whole = H.at[r, rows, :]
            lo, hi = H.at[r, rows, 0 : D // 2], H.at[r, rows, D // 2 : D]
            Pn[r][d] = [
                send(whole, whole, **{full: step(full, 1)}),
                send(whole, whole, **{full: step(full, 3)}),
                send(lo, lo, **{half: step(half, 1)}),
                send(hi, hi, **{half: step(half, 3)}),
            ]

    def to_sibling(r):
        for d in (1, 3, 2):
            for cp in Pn[r][d]:
                cp.wait_recv()
            xs = step("x", 4 - d)
            blk = hrows(r, c, xs, 0, 32)
            Cn[r][d] = send(blk, blk, c=oc)

    send_x(0)
    for d in (1, 3, 2):
        In[d] = send(IP.at[me], IP.at[me], x=step("x", d))
    Ic[0] = send(IP.at[me], IP.at[me], c=oc)
    send_x(1)
    forward(0)
    for d in (1, 3, 2):
        In[d].wait_recv()
        s = c * 4 + step("x", 4 - d)
        Ic[d] = send(IP.at[s], IP.at[s], c=oc)
    forward(1)
    to_sibling(0)
    for d in range(4):
        Ic[d].wait_recv()

    dp_index = x * 2 + c
    offset = (dp_index * 16 + y * 4 + z) * C
    SP = S["SP"]

    def sparse(r, lo, hi):
        def group(g, _):
            blk = g // 2
            j0 = r * 32 + (g % 2) * 16
            rows = pl.ds(pl.multiple_of(j0, 16), 16)
            local = IP[blk, rows, TOP : 2 * TOP].astype(jnp.int32) - offset
            local = jnp.where((local >= 0) & (local < C), local, -1).astype(jnp.int16)
            lane = lax.broadcasted_iota(jnp.int32, (16, 128), 1)
            n = -(-C // 128)
            cols = [(lane + 128 * k).astype(jnp.int16) for k in range(n)]
            acc = [jnp.full((16, 128), 127, jnp.int16) for _ in range(n)]
            for k in range(TOP):
                one = jnp.broadcast_to(local[:, k : k + 1], (16, 128))
                for j in range(n):
                    acc[j] = jnp.where(one == cols[j], jnp.int16(k), acc[j])
            for j in range(n):
                which = acc[j].astype(jnp.int32)
                wide = min(128, C - 128 * j)
                for s in range(2):
                    table = IP[blk, pl.ds(pl.multiple_of(j0 + s * 8, 8), 8), :]
                    sel = which[s * 8 : s * 8 + 8]
                    got = jnp.where(sel < TOP, jnp.take_along_axis(table, sel, axis=1), 0.0)
                    SP[r, pl.ds(pl.multiple_of(g * 16 + s * 8, 8), 8), 128 * j : 128 * j + wide] = got[:, :wide]
            return 0

        lax.fori_loop(lo, hi, group, 0)

    eye = (
        lax.broadcasted_iota(jnp.int32, (128, 128), 0) == lax.broadcasted_iota(jnp.int32, (128, 128), 1)
    )

    def to_row(col):
        return jnp.sum(jnp.where(eye, jnp.broadcast_to(col, (128, 128)), 0.0), axis=0, keepdims=True)

    def to_col(row):
        return jnp.sum(jnp.where(eye, jnp.broadcast_to(row, (128, 128)), 0.0), axis=1, keepdims=True)

    L, ST = S["L"], S["ST"]
    SA, SB = S["SA"], S["SB"]

    def spread(buf, r, slot, near):
        ref = buf.at[r, slot]
        if near:
            return [
                send(ref, ref, x=step("x", d), c=lax.rem(c + e, 2))
                for d in range(4) for e in range(2) if d or e
            ]
        return [
            send(ref, ref, y=step("y", d), z=step("z", e))
            for d in range(4) for e in range(4) if d or e
        ]

    def first_dot(r):
        L[r] = lax.dot_general(
            H[r], W[...], (((1,), (1,)), ((), ())), preferred_element_type=F32
        )

    def stats(r):
        def part(i, _):
            rows = pl.ds(pl.multiple_of(i * 32, 32), 32)
            v = L[r, rows, :]
            m = jnp.max(v, axis=1, keepdims=True)
            ST[rows, 0:1] = m
            ST[rows, 1:2] = jnp.sum(jnp.exp(v - m), axis=1, keepdims=True)
            return 0

        lax.fori_loop(0, 8, part, 0)
        for b in range(2):
            SA[r, me, b : b + 1, :] = to_row(ST[b * 128 : b * 128 + 128, 0:1])
            SA[r, me, b + 2 : b + 3, :] = to_row(ST[b * 128 : b * 128 + 128, 1:2])
        return spread(SA, r, me, True)

    def merged(buf, r, n, copies):
        for cp in copies:
            cp.wait_recv()
        m = buf[r, 0, 0:2, :]
        for k in range(1, n):
            m = jnp.maximum(m, buf[r, k, 0:2, :])
        s = jnp.zeros_like(m)
        for k in range(n):
            s = s + buf[r, k, 2:4, :] * jnp.exp(buf[r, k, 0:2, :] - m)
        return m, s

    plane = y * 4 + z

    def second_stats(r, copies):
        m, s = merged(SA, r, 8, copies)
        SB[r, plane, 0:2, :] = m
        SB[r, plane, 2:4, :] = s
        return spread(SB, r, plane, False)

    G, PK, LN = S["G"], S["PK"], S["LN"]

    def grads(r, copies):
        m, s = merged(SB, r, 16, copies)
        norm = m + jnp.log(s)
        for b in range(2):
            LN[r, b * 128 : b * 128 + 128, :] = to_col(norm[b : b + 1, :])

        def part(i, _):
            rows = pl.ds(pl.multiple_of(i * 32, 32), 32)
            v = L[r, rows, :]
            sp = SP[r, rows, :]
            mass = jnp.sum(IP[i, r * 32 : r * 32 + 32, 0:TOP], axis=1, keepdims=True)
            G[r, rows, :] = (mass * jnp.exp(v - LN[r, rows, :]) - sp).astype(BF16)
            PK[rows, :] = jnp.sum(sp * v, axis=1, keepdims=True)
            return 0

        lax.fori_loop(0, 8, part, 0)
        for b in range(2):
            S["QA"][r, me, b : b + 1, :] = to_row(PK[b * 128 : b * 128 + 128, :])

    PR, DS, DR = S["PR"], S["DS"], S["DR"]

    def second_dot(r, half):
        f0 = half * (D // 2)
        v = jnp.dot(G[r], W[:, f0 : f0 + D // 2], preferred_element_type=F32)
        for i in range(8):
            PR[r, half * 8 + i] = v[:, i * Z : i * Z + Z]

        def cast(i, _):
            DS[r, half * 8 + i] = PR[r, half * 8 + i, pl.ds(pl.multiple_of(oc * 128, 128), 128), :].astype(BF16)
            return 0

        lax.fori_loop(0, 8, cast, 0)
        part = pl.ds(half * 8, 8)
        return send(DS.at[r, part], DR.at[r, part], c=oc)

    def place(order, yg, zg, xb):
        of = {"x": xb, "y": yg, "z": zg}
        return tuple(of[a] for a in order)

    def phase1(r, copies):
        for cp in copies:
            cp.wait_recv()

        def part(i, _):
            yg, zg = i // 4, i % 4
            for xb in range(4):
                mine = pl.ds(pl.multiple_of(c * 128 + xb * 32, 32), 32)
                v = PR[r, i, mine, :] + DR[r, i, xb * 32 : xb * 32 + 32, :].astype(F32)
                PR[r, i, mine, :] = v
                for k, (order, rows) in enumerate(COLOURS):
                    p, q, s = place(order, yg, zg, xb)
                    r0, n = rows[r]
                    S[f"T1{r}{k}"][p, q * 4 + s] = v[r0 : r0 + n].astype(BF16)
            return 0

        lax.fori_loop(0, 16, part, 0)
        res = []
        for k, (order, _) in enumerate(COLOURS):
            a = order[0]
            T, R = S[f"T1{r}{k}"], S[f"R1{r}{k}"]
            res.append([send(T.at[step(a, d)], R.at[d - 1], **{a: step(a, d)}) for d in (1, 3, 2)])
        return res

    def phase2(r, copies):
        res = []
        for k, (order, rows) in enumerate(COLOURS):
            for cp in copies[k]:
                cp.wait_recv()
            a, b, _ = order
            r0, n = rows[r]
            R, T = S[f"R1{r}{k}"], S[f"T2{r}{k}"]

            def part(i, _, order=order, r0=r0, n=n, R=R, T=T):
                at = dict(zip(order, (co[order[0]], i // 4, i % 4)))
                row = pl.ds(pl.multiple_of(c * 128 + at["x"] * 32 + r0, 8), n)
                v = PR[r, at["y"] * 4 + at["z"], row, :]
                for d in range(3):
                    v = v + R[d, i].astype(F32)
                T[i // 4, i % 4] = v.astype(T.dtype)
                return 0

            lax.fori_loop(0, 16, part, 0)
            R2 = S[f"R2{r}{k}"]
            res.append([send(T.at[step(b, d)], R2.at[d - 1], **{b: step(b, d)}) for d in (1, 3, 2)])
        return res

    def phase3(r, copies):
        res = []
        for k, (order, rows) in enumerate(COLOURS):
            for cp in copies[k]:
                cp.wait_recv()
            _, b, e = order
            T2, R2, T3, R3 = S[f"T2{r}{k}"], S[f"R2{r}{k}"], S[f"T3{r}{k}"], S[f"R3{r}{k}"]
            for s in range(4):
                v = T2[co[b], s].astype(F32)
                for d in range(3):
                    v = v + R2[d, s].astype(F32)
                T3[s] = v
            res.append([send(T3.at[step(e, d)], R3.at[d - 1], **{e: step(e, d)}) for d in (1, 3, 2)])
        return res

    def finish(r, copies, weight):
        for k, (order, rows) in enumerate(COLOURS):
            for cp in copies[k]:
                cp.wait_recv()
            r0, n = rows[r]
            T3, R3 = S[f"T3{r}{k}"], S[f"R3{r}{k}"]
            v = T3[co[order[2]]]
            for d in range(3):
                v = v + R3[d]
            lo = r * 32 + r0
            out[lo : lo + n, :] = weight[lo : lo + n, :] * v

    QA, QB = S["QA"], S["QB"]

    sparse(0, 0, 8)
    to_sibling(1)
    sparse(0, 8, 16)
    wcopy.wait()
    for d in range(4):
        Cn[0][d].wait_recv()
    first_dot(0)
    a0 = stats(0)
    for d in range(4):
        Cn[1][d].wait_recv()
    first_dot(1)
    b0 = second_stats(0, a0)
    a1 = stats(1)
    sparse(1, 0, 16)
    b1 = second_stats(1, a1)
    grads(0, b0)
    d0 = [second_dot(0, 0), second_dot(0, 1)]
    grads(1, b1)
    p0 = phase1(0, d0)
    d1 = [second_dot(1, 0), second_dot(1, 1)]
    qa = spread(QA, 0, me, True) + spread(QA, 1, me, True)
    p1 = phase1(1, d1)
    p0 = phase2(0, p0)
    for cp in qa:
        cp.wait_recv()
    for r in range(2):
        tot = QA[r, 0]
        for k in range(1, 8):
            tot = tot + QA[r, k]
        QB[r, plane] = tot
    qb = spread(QB, 0, plane, False) + spread(QB, 1, plane, False)
    p1 = phase2(1, p1)
    p0 = phase3(0, p0)
    p1 = phase3(1, p1)

    small = (
        lax.broadcasted_iota(jnp.int32, (64, 64), 0) == lax.broadcasted_iota(jnp.int32, (64, 64), 1)
    )
    weight = jnp.sum(jnp.where(small, jnp.broadcast_to(tw[...], (64, 64)), 0.0), axis=1, keepdims=True)
    for cp in qb:
        cp.wait_recv()
    for r in range(2):
        tot = QB[r, 0]
        for k in range(1, 16):
            tot = tot + QB[r, k]
        for b in range(2):
            PK[b * 128 : b * 128 + 128, :] = to_col(tot[b : b + 1, :])
        mine = pl.ds(pl.multiple_of(me * 32, 32), 32)
        q = pr[r * 32 : r * 32 + 32, :]
        mass = jnp.sum(q, axis=1, keepdims=True)
        S["DV"][r * 32 : r * 32 + 32, :] = (
            jnp.sum(q * jnp.log(q), axis=1, keepdims=True) - PK[mine, :] + mass * LN[r, mine, :]
        )
    dv[...] = jnp.sum(jnp.where(small, jnp.broadcast_to(S["DV"][...], (64, 64)), 0.0), axis=0, keepdims=True)
    finish(0, p0, weight)
    finish(1, p1, weight)
    for cp in sent:
        cp.wait_send()


def body(hidden, head_weight, teacher_ids, teacher_probs, token_weight):
    T, D = hidden.shape
    C = head_weight.shape[1]
    Z = D // 16
    V = pltpu.VMEM
    scratch = {
        "W": V((C, D), BF16), "H": V((2, 256, D), BF16), "IP": V((8, T, 128), F32),
        "SP": V((2, 256, C), F32), "L": V((2, 256, C), F32), "ST": V((256, 2), F32),
        "SA": V((2, 8, 8, 128), F32), "SB": V((2, 16, 8, 128), F32),
        "QA": V((2, 8, 8, 128), F32), "QB": V((2, 16, 8, 128), F32),
        "G": V((2, 256, C), BF16), "PK": V((256, 1), F32), "LN": V((2, 256, 1), F32),
        "DV": V((T, 1), F32),
        "PR": V((2, 16, 256, Z), F32), "DS": V((2, 16, 128, Z), BF16), "DR": V((2, 16, 128, Z), BF16),
    }
    for r in range(2):
        for k, (_, rows) in enumerate(COLOURS):
            n = rows[r][1]
            scratch[f"T1{r}{k}"] = V((4, 16, n, Z), BF16)
            scratch[f"R1{r}{k}"] = V((3, 16, n, Z), BF16)
            scratch[f"T2{r}{k}"] = V((4, 4, n, Z), WIRE2)
            scratch[f"R2{r}{k}"] = V((3, 4, n, Z), WIRE2)
            scratch[f"T3{r}{k}"] = V((4, n, Z), F32)
            scratch[f"R3{r}{k}"] = V((3, n, Z), F32)
    scratch["ss"] = pltpu.SemaphoreType.DMA((220,))
    scratch["rs"] = pltpu.SemaphoreType.DMA((220,))
    scratch["ws"] = pltpu.SemaphoreType.DMA
    vm = pl.BlockSpec(memory_space=pltpu.VMEM)
    grad, div = pl.pallas_call(
        functools.partial(kernel, names=tuple(scratch)),
        out_shape=(jax.ShapeDtypeStruct((T, Z), F32), jax.ShapeDtypeStruct((1, T), F32)),
        in_specs=[vm, pl.BlockSpec(memory_space=pl.ANY), vm, vm, vm],
        out_specs=(vm, vm),
        scratch_shapes=list(scratch.values()),
        compiler_params=pltpu.CompilerParams(
            collective_id=0, has_side_effects=True, vmem_limit_bytes=67043328
        ),
        name="distill",
    )(hidden, head_weight.T, teacher_ids, teacher_probs, token_weight.reshape(1, T))
    return div.reshape(T), grad


def solution(mesh):
    split = Mesh(mesh.devices.reshape(4, 2, 4, 4), ("x", "c", "y", "z"))
    placed = (P(DP, None), P(None, DP + VOCAB), P(DP, None), P(DP, None), P(DP))
    return jax.shard_map(
        body, mesh=split, in_specs=placed, out_specs=(P(DP), P(DP, VOCAB)), check_vma=False
    )
```

```python
import functools

import jax
import jax.numpy as jnp
from jax import lax
from jax.experimental import pallas as pl
from jax.experimental.pallas import tpu as pltpu
from jax.sharding import Mesh
from jax.sharding import PartitionSpec as P

MESH = pl.DeviceIdType.MESH
DP = ("x", "c")
VOCAB = ("y", "z")
F32 = jnp.float32
BF16 = jnp.bfloat16
COLOURS = (
    (("x", "y", "z"), (((0, 0), (0, 1), (3, 0)), ((0, 0), (0, 1)))),
    (("y", "z", "x"), (((1, 0), (1, 1), (3, 1)), ((1, 0), (1, 1), (3, 0)))),
    (("z", "x", "y"), (((2, 0), (2, 1)), ((2, 0), (2, 1), (3, 1)))),
)


def kernel(h, w, ids_in, pr_in, tw_in, out, dv, *scratch, names):
    S = dict(zip(names, scratch))
    D = h.shape[1]
    C = w.shape[0]
    TOP = ids_in.shape[1]
    Z = D // 16
    co = {a: lax.axis_index(a) for a in ("x", "c", "y", "z")}
    x, c, y, z = co["x"], co["c"], co["y"], co["z"]
    oc = 1 - c
    count = [0]

    def step(axis, d):
        return lax.rem(co[axis] + d, 4)

    def send(src, dst, **dev):
        i = count[0]
        count[0] += 1
        cp = pltpu.make_async_remote_copy(
            src_ref=src, dst_ref=dst, send_sem=S["ss"].at[i], recv_sem=S["rs"].at[i],
            device_id=dev, device_id_type=MESH,
        )
        cp.start()
        sent.append(cp)
        return cp

    sent = []
    bar = pltpu.get_barrier_semaphore()
    for d in range(4):
        for e in range(2):
            if d or e:
                pl.semaphore_signal(
                    bar, inc=1, device_id={"x": step("x", d), "c": lax.rem(c + e, 2)}, device_id_type=MESH
                )
    for d in range(4):
        for e in range(4):
            if d or e:
                pl.semaphore_signal(
                    bar, inc=1, device_id={"y": step("y", d), "z": step("z", e)}, device_id_type=MESH
                )
    H, IP, W = S["H"], S["IP"], S["W"]
    me = c * 4 + x
    own = pl.ds(pl.multiple_of(me * 32, 32), 32)
    ids, pr, tw = S["ids"], S["pr"], S["tw"]
    local = [
        pltpu.make_async_copy(ids_in, ids, S["ls"].at[0]),
        pltpu.make_async_copy(pr_in, pr, S["ls"].at[1]),
        pltpu.make_async_copy(h.at[0:32, :], H.at[0, own, :], S["ls"].at[2]),
        pltpu.make_async_copy(h.at[32:64, :], H.at[1, own, :], S["ls"].at[3]),
        pltpu.make_async_copy(w, W, S["ls"].at[4]),
        pltpu.make_async_copy(tw_in, tw, S["ls"].at[5]),
    ]
    for cp in local:
        cp.start()
    for cp in local[:2]:
        cp.wait()
    IP[me, :, 0:TOP] = pr[...]
    IP[me, :, TOP : 2 * TOP] = ids[...].astype(F32)
    for cp in local[2:4]:
        cp.wait()
    pl.semaphore_wait(bar, 22)

    share = (lax.rem(y + 2 * z, 4), lax.rem(2 * y + z, 4))
    X, Pn, Cn, In, Ic = [{}, {}], [{}, {}], [{}, {}], {}, {}

    def hrows(r, core, xb, off, n):
        return H.at[r, pl.ds(pl.multiple_of(core * 128 + xb * 32 + off, 8), n), :]

    def send_x(r):
        for d in (1, 3, 2):
            part = hrows(r, c, x, share[r] * 8, 8)
            X[r][d] = send(part, part, x=step("x", d))
        whole = hrows(r, c, x, 0, 32)
        Cn[r][0] = send(whole, whole, c=oc)

    def forward(r):
        full, half = (("y", "z"), ("z", "y"))[r]
        for d in (1, 3, 2):
            X[r][d].wait_recv()
            xs = step("x", 4 - d)
            rows = pl.ds(pl.multiple_of(c * 128 + xs * 32 + share[r] * 8, 8), 8)
            whole = H.at[r, rows, :]
            lo, hi = H.at[r, rows, 0 : D // 2], H.at[r, rows, D // 2 : D]
            Pn[r][d] = [
                send(whole, whole, **{full: step(full, 1)}),
                send(whole, whole, **{full: step(full, 3)}),
                send(lo, lo, **{half: step(half, 1)}),
                send(hi, hi, **{half: step(half, 3)}),
            ]

    def to_sibling(r):
        for d in (1, 3, 2):
            for cp in Pn[r][d]:
                cp.wait_recv()
            xs = step("x", 4 - d)
            blk = hrows(r, c, xs, 0, 32)
            Cn[r][d] = send(blk, blk, c=oc)

    dp_index = x * 2 + c
    offset = (dp_index * 16 + y * 4 + z) * C
    SP = S["SP"]

    def sparse(r, lo, hi):
        def group(g, _):
            blk = g // 2
            j0 = r * 32 + (g % 2) * 16
            rows = pl.ds(pl.multiple_of(j0, 16), 16)
            local = IP[blk, rows, TOP : 2 * TOP].astype(jnp.int32) - offset
            local = jnp.where((local >= 0) & (local < C), local, -1).astype(jnp.int16)
            lane = lax.broadcasted_iota(jnp.int32, (16, 128), 1)
            n = -(-C // 128)
            cols = [(lane + 128 * k).astype(jnp.int16) for k in range(n)]
            acc = [jnp.full((16, 128), 127, jnp.int16) for _ in range(n)]
            for k in range(TOP):
                one = jnp.broadcast_to(local[:, k : k + 1], (16, 128))
                for j in range(n):
                    acc[j] = jnp.where(one == cols[j], jnp.int16(k), acc[j])
            for j in range(n):
                which = acc[j].astype(jnp.int32)
                wide = min(128, C - 128 * j)
                for s in range(2):
                    table = IP[blk, pl.ds(pl.multiple_of(j0 + s * 8, 8), 8), :]
                    sel = which[s * 8 : s * 8 + 8]
                    got = jnp.where(sel < TOP, jnp.take_along_axis(table, sel, axis=1), 0.0)
                    SP[r, pl.ds(pl.multiple_of(g * 16 + s * 8, 8), 8), 128 * j : 128 * j + wide] = got[:, :wide]
            return 0

        lax.fori_loop(lo, hi, group, 0)

    eye = (
        lax.broadcasted_iota(jnp.int32, (128, 128), 0) == lax.broadcasted_iota(jnp.int32, (128, 128), 1)
    )

    def to_row(col):
        return jnp.sum(jnp.where(eye, jnp.broadcast_to(col, (128, 128)), 0.0), axis=0, keepdims=True)

    def to_col(row):
        return jnp.sum(jnp.where(eye, jnp.broadcast_to(row, (128, 128)), 0.0), axis=1, keepdims=True)

    L, ST = S["L"], S["ST"]
    SA, SB = S["SA"], S["SB"]

    def spread(ref, near):
        if near:
            return [
                send(ref, ref, x=step("x", d), c=lax.rem(c + e, 2))
                for d in range(4) for e in range(2) if d or e
            ]
        return [
            send(ref, ref, y=step("y", d), z=step("z", e))
            for d in range(4) for e in range(4) if d or e
        ]

    def first_dot(r):
        L[r] = lax.dot_general(
            H[r], W[...], (((1,), (1,)), ((), ())), preferred_element_type=F32
        )

    def stats(r):
        def part(i, _):
            rows = pl.ds(pl.multiple_of(i * 32, 32), 32)
            v = L[r, rows, :]
            m = jnp.max(v, axis=1, keepdims=True)
            ST[rows, 0:1] = m
            ST[rows, 1:2] = jnp.sum(jnp.exp(v - m), axis=1, keepdims=True)
            return 0

        lax.fori_loop(0, 8, part, 0)
        for b in range(2):
            SA[r, me, b : b + 1, :] = to_row(ST[b * 128 : b * 128 + 128, 0:1])
            SA[r, me, b + 2 : b + 3, :] = to_row(ST[b * 128 : b * 128 + 128, 1:2])
        return spread(SA.at[r, me], True)

    def merged(buf, r, n, copies):
        for cp in copies:
            cp.wait_recv()
        m = buf[r, 0, 0:2, :]
        for k in range(1, n):
            m = jnp.maximum(m, buf[r, k, 0:2, :])
        s = jnp.zeros_like(m)
        for k in range(n):
            s = s + buf[r, k, 2:4, :] * jnp.exp(buf[r, k, 0:2, :] - m)
        return m, s

    plane = y * 4 + z

    def second_stats(r, copies):
        m, s = merged(SA, r, 8, copies)
        SB[r, plane, 0:2, :] = m
        SB[r, plane, 2:4, :] = s
        return spread(SB.at[r, plane], False)

    G, PK, LN, QA, QB = S["G"], S["PK"], S["LN"], S["QA"], S["QB"]

    def grads(r, copies):
        m, s = merged(SB, r, 16, copies)
        norm = m + jnp.log(s)
        for b in range(2):
            LN[r, b * 128 : b * 128 + 128, :] = to_col(norm[b : b + 1, :])

        def part(i, _):
            rows = pl.ds(pl.multiple_of(i * 32, 32), 32)
            v = L[r, rows, :]
            sp = SP[r, rows, :]
            mass = jnp.sum(IP[i, r * 32 : r * 32 + 32, 0:TOP], axis=1, keepdims=True)
            G[r, rows, :] = (mass * jnp.exp(v - LN[r, rows, :]) - sp).astype(BF16)
            PK[rows, :] = jnp.sum(sp * v, axis=1, keepdims=True)
            return 0

        lax.fori_loop(0, 8, part, 0)
        for b in range(2):
            QA[me, 2 * r + b : 2 * r + b + 1, :] = to_row(PK[b * 128 : b * 128 + 128, :])

    PR, DS, DR = S["PR"], S["DS"], S["DR"]

    def second_dot(r):
        v = jnp.dot(G[r, pl.ds(pl.multiple_of(oc * 128, 128), 128), :], W[...], preferred_element_type=F32)
        for i in range(16):
            DS[r, i, :, 0:Z] = v[:, i * Z : i * Z + Z].astype(BF16)
        cp = send(DS.at[r], DR.at[r], c=oc)
        v = jnp.dot(G[r, pl.ds(pl.multiple_of(c * 128, 128), 128), :], W[...], preferred_element_type=F32)
        for i in range(16):
            PR[r, i, :, 0:Z] = v[:, i * Z : i * Z + Z]
        return cp

    def place(order, yg, zg, xb):
        of = {"x": xb, "y": yg, "z": zg}
        return tuple(of[a] for a in order)

    def phase1(r, copy):
        copy.wait_recv()

        def part(i, _):
            yg, zg = i // 4, i % 4
            for xb in range(4):
                rows = pl.ds(xb * 32, 32)
                v = PR[r, i, rows, :] + DR[r, i, rows, :].astype(F32)
                PR[r, i, rows, :] = v
                for k, (order, tiles) in enumerate(COLOURS):
                    p, q, s = place(order, yg, zg, xb)
                    for t, (rb, lt) in enumerate(tiles[r]):
                        S[f"T1{r}{k}"][p, q * 4 + s, t] = v[rb * 8 : rb * 8 + 8, lt * 128 : lt * 128 + 128].astype(BF16)
            return 0

        lax.fori_loop(0, 16, part, 0)
        res = []
        for k, (order, _) in enumerate(COLOURS):
            a = order[0]
            T, R = S[f"T1{r}{k}"], S[f"R1{r}{k}"]
            res.append([send(T.at[step(a, d)], R.at[d - 1], **{a: step(a, d)}) for d in (1, 3, 2)])
        return res

    def phase2(r, copies):
        res = []
        for k, (order, tiles) in enumerate(COLOURS):
            for cp in copies[k]:
                cp.wait_recv()
            a, b, e = order
            R, T = S[f"R1{r}{k}"], S[f"T2{r}{k}"]

            def part(i, _, order=order, tiles=tiles[r], R=R, T=T):
                at = dict(zip(order, (co[order[0]], i // 4, i % 4)))
                for t, (rb, lt) in enumerate(tiles):
                    rows = pl.ds(pl.multiple_of(at["x"] * 32 + rb * 8, 8), 8)
                    v = PR[r, at["y"] * 4 + at["z"], rows, lt * 128 : lt * 128 + 128]
                    for d in range(3):
                        v = v + R[d, i, t].astype(F32)
                    T[i, t] = v.astype(BF16)
                return 0

            lax.fori_loop(0, 16, part, 0)
            R2 = S[f"R2{r}{k}"]
            res.append([
                send(T.at[step(b, d) * 4 + step(e, f)], R2.at[d * 4 + f - 1], **{b: step(b, d), e: step(e, f)})
                for d in range(4) for f in range(4) if d or f
            ])
        return res

    def finish(r, copies, weight):
        for k, (order, tiles) in enumerate(COLOURS):
            for cp in copies[k]:
                cp.wait_recv()
            _, b, e = order
            T2, R2 = S[f"T2{r}{k}"], S[f"R2{r}{k}"]
            for t, (rb, lt) in enumerate(tiles[r]):
                v = T2[co[b] * 4 + co[e], t].astype(F32)
                for j in range(15):
                    v = v + R2[j, t].astype(F32)
                lo, wide = r * 32 + rb * 8, min(128, Z - lt * 128)
                out[lo : lo + 8, lt * 128 : lt * 128 + wide] = weight[lo : lo + 8, :] * v[:, :wide]

    for d in (1, 3, 2):
        In[d] = send(IP.at[me], IP.at[me], x=step("x", d))
    send_x(0)
    send_x(1)
    Ic[0] = send(IP.at[me], IP.at[me], c=oc)
    for d in (1, 3, 2):
        In[d].wait_recv()
        s = c * 4 + step("x", 4 - d)
        Ic[d] = send(IP.at[s], IP.at[s], c=oc)
    for d in range(4):
        Ic[d].wait_recv()
    sparse(0, 0, 2)
    forward(0)
    sparse(0, 2, 8)
    forward(1)
    sparse(0, 8, 12)
    to_sibling(0)
    sparse(0, 12, 16)
    local[4].wait()
    for d in range(4):
        Cn[0][d].wait_recv()
    first_dot(0)
    to_sibling(1)
    a0 = stats(0)
    for d in range(4):
        Cn[1][d].wait_recv()
    first_dot(1)
    b0 = second_stats(0, a0)
    a1 = stats(1)
    sparse(1, 0, 8)
    b1 = second_stats(1, a1)
    sparse(1, 8, 16)
    grads(0, b0)
    p0 = second_dot(0)
    grads(1, b1)
    p0 = phase1(0, p0)
    p1 = second_dot(1)
    p1 = phase1(1, p1)
    qa = spread(QA.at[me], True)
    p0 = phase2(0, p0)
    for cp in qa:
        cp.wait_recv()
    tot = QA[0]
    for k in range(1, 8):
        tot = tot + QA[k]
    QB[plane] = tot
    qb = spread(QB.at[plane], False)
    p1 = phase2(1, p1)

    local[5].wait()
    small = (
        lax.broadcasted_iota(jnp.int32, (64, 64), 0) == lax.broadcasted_iota(jnp.int32, (64, 64), 1)
    )
    weight = jnp.sum(jnp.where(small, jnp.broadcast_to(tw[...], (64, 64)), 0.0), axis=1, keepdims=True)
    for cp in qb:
        cp.wait_recv()
    tot = QB[0]
    for k in range(1, 16):
        tot = tot + QB[k]
    for r in range(2):
        for b in range(2):
            PK[b * 128 : b * 128 + 128, :] = to_col(tot[2 * r + b : 2 * r + b + 1, :])
        q = pr[r * 32 : r * 32 + 32, :]
        mass = jnp.sum(q, axis=1, keepdims=True)
        S["DV"][r * 32 : r * 32 + 32, :] = (
            jnp.sum(q * jnp.log(q), axis=1, keepdims=True) - PK[own, :] + mass * LN[r, own, :]
        )
    dv[...] = jnp.sum(jnp.where(small, jnp.broadcast_to(S["DV"][...], (64, 64)), 0.0), axis=0, keepdims=True)
    finish(0, p0, weight)
    finish(1, p1, weight)
    for cp in sent:
        cp.wait_send()


def body(hidden, head_weight, teacher_ids, teacher_probs, token_weight):
    T, D = hidden.shape
    C = head_weight.shape[1]
    Z = D // 16
    V = pltpu.VMEM
    scratch = {
        "W": V((C, D), BF16), "H": V((2, 256, D), BF16), "IP": V((8, T, 128), F32),
        "SP": V((2, 256, C), F32), "L": V((2, 256, C), F32), "ST": V((256, 2), F32),
        "SA": V((2, 8, 8, 128), F32), "SB": V((2, 16, 8, 128), F32),
        "QA": V((8, 8, 128), F32), "QB": V((16, 8, 128), F32),
        "G": V((2, 256, C), BF16), "PK": V((256, 1), F32), "LN": V((2, 256, 1), F32),
        "DV": V((T, 1), F32),
        "PR": V((2, 16, 128, 256), F32), "DS": V((2, 16, 128, 256), BF16), "DR": V((2, 16, 128, 256), BF16),
        "ids": V(teacher_ids.shape, jnp.int32), "pr": V(teacher_probs.shape, F32), "tw": V((1, T), F32),
    }
    for r in range(2):
        for k, (_, tiles) in enumerate(COLOURS):
            n = len(tiles[r])
            scratch[f"T1{r}{k}"] = V((4, 16, n, 8, 128), BF16)
            scratch[f"R1{r}{k}"] = V((3, 16, n, 8, 128), BF16)
            scratch[f"T2{r}{k}"] = V((16, n, 8, 128), BF16)
            scratch[f"R2{r}{k}"] = V((15, n, 8, 128), BF16)
    scratch["ss"] = pltpu.SemaphoreType.DMA((224,))
    scratch["rs"] = pltpu.SemaphoreType.DMA((224,))
    scratch["ls"] = pltpu.SemaphoreType.DMA((6,))
    vm = pl.BlockSpec(memory_space=pltpu.VMEM)
    grad, div = pl.pallas_call(
        functools.partial(kernel, names=tuple(scratch)),
        out_shape=(jax.ShapeDtypeStruct((T, Z), F32), jax.ShapeDtypeStruct((1, T), F32)),
        in_specs=[pl.BlockSpec(memory_space=pl.ANY)] * 5,
        out_specs=(vm, vm),
        scratch_shapes=list(scratch.values()),
        compiler_params=pltpu.CompilerParams(
            collective_id=0, has_side_effects=True, vmem_limit_bytes=67043328
        ),
        name="distill",
    )(hidden, head_weight.T, teacher_ids, teacher_probs, token_weight.reshape(1, T))
    return div.reshape(T), grad


def solution(mesh):
    split = Mesh(mesh.devices.reshape(4, 2, 4, 4), ("x", "c", "y", "z"))
    placed = (P(DP, None), P(None, DP + VOCAB), P(DP, None), P(DP, None), P(DP))
    return jax.shard_map(
        body, mesh=split, in_specs=placed, out_specs=(P(DP), P(DP, VOCAB)), check_vma=False
    )
```

```python
import functools

import jax
import jax.numpy as jnp
from jax import lax
from jax.experimental import pallas as pl
from jax.experimental.pallas import tpu as pltpu
from jax.sharding import Mesh
from jax.sharding import PartitionSpec as P

MESH = pl.DeviceIdType.MESH
DP = ("x", "c")
VOCAB = ("y", "z")
F32 = jnp.float32
BF16 = jnp.bfloat16
COLOURS = (
    (("x", "y", "z"), (((0, 0), (0, 1), (3, 0)), ((0, 0), (0, 1)))),
    (("y", "z", "x"), (((1, 0), (1, 1), (3, 1)), ((1, 0), (1, 1), (3, 0)))),
    (("z", "x", "y"), (((2, 0), (2, 1)), ((2, 0), (2, 1), (3, 1)))),
)


def kernel(h, w, ids_in, pr_in, tw_in, out, dv, *scratch, names):
    S = dict(zip(names, scratch))
    D = h.shape[1]
    C = w.shape[0]
    TOP = ids_in.shape[1]
    Z = D // 16
    co = {a: lax.axis_index(a) for a in ("x", "c", "y", "z")}
    x, c, y, z = co["x"], co["c"], co["y"], co["z"]
    oc = 1 - c
    count = [0]

    def step(axis, d):
        return lax.rem(co[axis] + d, 4)

    def send(src, dst, **dev):
        i = count[0]
        count[0] += 1
        cp = pltpu.make_async_remote_copy(
            src_ref=src, dst_ref=dst, send_sem=S["ss"].at[i], recv_sem=S["rs"].at[i],
            device_id=dev, device_id_type=MESH,
        )
        cp.start()
        sent.append(cp)
        return cp

    sent = []
    bar = pltpu.get_barrier_semaphore()
    for d in range(4):
        for e in range(2):
            if d or e:
                pl.semaphore_signal(
                    bar, inc=1, device_id={"x": step("x", d), "c": lax.rem(c + e, 2)}, device_id_type=MESH
                )
    beside = [{"y": step("y", 1)}, {"y": step("y", 3)}, {"z": step("z", 1)}, {"z": step("z", 3)}]
    for dev in beside:
        pl.semaphore_signal(bar, inc=1, device_id=dev, device_id_type=MESH)
    H, IP, W = S["H"], S["IP"], S["W"]
    me = c * 4 + x
    own = pl.ds(pl.multiple_of(me * 32, 32), 32)
    ids, pr, tw = S["ids"], S["pr"], S["tw"]
    local = [
        pltpu.make_async_copy(ids_in, ids, S["ls"].at[0]),
        pltpu.make_async_copy(pr_in, pr, S["ls"].at[1]),
        pltpu.make_async_copy(h.at[0:32, :], H.at[0, own, :], S["ls"].at[2]),
        pltpu.make_async_copy(h.at[32:64, :], H.at[1, own, :], S["ls"].at[3]),
        pltpu.make_async_copy(w, W, S["ls"].at[4]),
        pltpu.make_async_copy(tw_in, tw, S["ls"].at[5]),
    ]
    for cp in local:
        cp.start()
    for cp in local[:2]:
        cp.wait()
    IP[me, :, 0:TOP] = pr[...]
    IP[me, :, TOP : 2 * TOP] = ids[...].astype(F32)
    for cp in local[2:4]:
        cp.wait()
    pl.semaphore_wait(bar, 11)

    def tell(i):
        for dev in beside:
            pl.semaphore_signal(S["hs"].at[i], inc=1, device_id=dev, device_id_type=MESH)

    def hear(i):
        pl.semaphore_wait(S["hs"].at[i], 4)

    share = (lax.rem(y + 2 * z, 4), lax.rem(2 * y + z, 4))
    X, Pn, Cn, In, Ic = [{}, {}], [{}, {}], [{}, {}], {}, {}

    def hrows(r, core, xb, off, n):
        return H.at[r, pl.ds(pl.multiple_of(core * 128 + xb * 32 + off, 8), n), :]

    def send_x(r):
        for d in (1, 3, 2):
            X[r][d] = []
            for half in range(2):
                rows = pl.ds(pl.multiple_of(me * 32 + share[half] * 8, 8), 8)
                part = H.at[r, rows, half * (D // 2) : (half + 1) * (D // 2)]
                X[r][d].append(send(part, part, x=step("x", d)))
        whole = hrows(r, c, x, 0, 32)
        Cn[r][0] = send(whole, whole, c=oc)

    def forward(r):
        for d in (1, 3, 2):
            xs = step("x", 4 - d)
            Pn[r][d] = []
            for half in range(2):
                X[r][d][half].wait_recv()
                more, less = (("y", "z"), ("z", "y"))[half]
                rows = pl.ds(pl.multiple_of(c * 128 + xs * 32 + share[half] * 8, 8), 8)
                at = half * (D // 2)
                whole = H.at[r, rows, at : at + D // 2]
                lo, hi = H.at[r, rows, at : at + D // 4], H.at[r, rows, at + D // 4 : at + D // 2]
                Pn[r][d] += [
                    send(whole, whole, **{more: step(more, 1)}),
                    send(whole, whole, **{more: step(more, 3)}),
                    send(lo, lo, **{less: step(less, 1)}),
                    send(hi, hi, **{less: step(less, 3)}),
                ]

    def to_sibling(r):
        for d in (1, 3, 2):
            for cp in Pn[r][d]:
                cp.wait_recv()
            xs = step("x", 4 - d)
            blk = hrows(r, c, xs, 0, 32)
            Cn[r][d] = send(blk, blk, c=oc)

    dp_index = x * 2 + c
    offset = (dp_index * 16 + y * 4 + z) * C
    SP = S["SP"]

    def sparse(r, blk):
        def group(i, _):
            g = blk * 2 + i
            j0 = r * 32 + i * 16
            rows = pl.ds(pl.multiple_of(j0, 16), 16)
            local = IP[blk, rows, TOP : 2 * TOP].astype(jnp.int32) - offset
            local = jnp.where((local >= 0) & (local < C), local, -1).astype(jnp.int16)
            lane = lax.broadcasted_iota(jnp.int32, (16, 128), 1)
            n = -(-C // 128)
            cols = [(lane + 128 * k).astype(jnp.int16) for k in range(n)]
            acc = [jnp.full((16, 128), 127, jnp.int16) for _ in range(n)]
            for k in range(TOP):
                one = jnp.broadcast_to(local[:, k : k + 1], (16, 128))
                for j in range(n):
                    acc[j] = jnp.where(one == cols[j], jnp.int16(k), acc[j])
            for j in range(n):
                which = acc[j].astype(jnp.int32)
                wide = min(128, C - 128 * j)
                for s in range(2):
                    table = IP[blk, pl.ds(pl.multiple_of(j0 + s * 8, 8), 8), :]
                    sel = which[s * 8 : s * 8 + 8]
                    got = jnp.where(sel < TOP, jnp.take_along_axis(table, sel, axis=1), 0.0)
                    SP[r, pl.ds(pl.multiple_of(g * 16 + s * 8, 8), 8), 128 * j : 128 * j + wide] = got[:, :wide]
            return 0

        lax.fori_loop(0, 2, group, 0)

    eye = (
        lax.broadcasted_iota(jnp.int32, (128, 128), 0) == lax.broadcasted_iota(jnp.int32, (128, 128), 1)
    )

    def to_row(col):
        return jnp.sum(jnp.where(eye, jnp.broadcast_to(col, (128, 128)), 0.0), axis=0, keepdims=True)

    def to_col(row):
        return jnp.sum(jnp.where(eye, jnp.broadcast_to(row, (128, 128)), 0.0), axis=1, keepdims=True)

    L, ST = S["L"], S["ST"]
    SA, SB = S["SA"], S["SB"]

    def spread(ref, near):
        if near:
            return [
                send(ref, ref, x=step("x", d), c=lax.rem(c + e, 2))
                for d in range(4) for e in range(2) if d or e
            ]
        return [
            send(ref, ref, y=step("y", d), z=step("z", e))
            for d in range(4) for e in range(4) if d or e
        ]

    def first_dot(r):
        L[r] = lax.dot_general(
            H[r], W[...], (((1,), (1,)), ((), ())), preferred_element_type=F32
        )

    def stats(r):
        def part(i, _):
            rows = pl.ds(pl.multiple_of(i * 32, 32), 32)
            v = L[r, rows, :]
            m = jnp.max(v, axis=1, keepdims=True)
            ST[rows, 0:1] = m
            ST[rows, 1:2] = jnp.sum(jnp.exp(v - m), axis=1, keepdims=True)
            return 0

        lax.fori_loop(0, 8, part, 0)
        for b in range(2):
            SA[r, me, b : b + 1, :] = to_row(ST[b * 128 : b * 128 + 128, 0:1])
            SA[r, me, b + 2 : b + 3, :] = to_row(ST[b * 128 : b * 128 + 128, 1:2])
        return spread(SA.at[r, me], True)

    def merged(buf, r, n, copies):
        for cp in copies:
            cp.wait_recv()
        m = buf[r, 0, 0:2, :]
        for k in range(1, n):
            m = jnp.maximum(m, buf[r, k, 0:2, :])
        s = jnp.zeros_like(m)
        for k in range(n):
            s = s + buf[r, k, 2:4, :] * jnp.exp(buf[r, k, 0:2, :] - m)
        return m, s

    plane = y * 4 + z

    def second_stats(r, copies):
        m, s = merged(SA, r, 8, copies)
        SB[r, plane, 0:2, :] = m
        SB[r, plane, 2:4, :] = s
        return spread(SB.at[r, plane], False)

    G, PK, LN, QA, QB = S["G"], S["PK"], S["LN"], S["QA"], S["QB"]

    def grads(r, copies):
        m, s = merged(SB, r, 16, copies)
        norm = m + jnp.log(s)
        for b in range(2):
            LN[r, b * 128 : b * 128 + 128, :] = to_col(norm[b : b + 1, :])

        def part(i, _):
            rows = pl.ds(pl.multiple_of(i * 32, 32), 32)
            v = L[r, rows, :]
            sp = SP[r, rows, :]
            mass = jnp.sum(IP[i, r * 32 : r * 32 + 32, 0:TOP], axis=1, keepdims=True)
            G[r, rows, :] = (mass * jnp.exp(v - LN[r, rows, :]) - sp).astype(BF16)
            PK[rows, :] = jnp.sum(sp * v, axis=1, keepdims=True)
            return 0

        lax.fori_loop(0, 8, part, 0)
        for b in range(2):
            QA[me, 2 * r + b : 2 * r + b + 1, :] = to_row(PK[b * 128 : b * 128 + 128, :])

    PR, DS, DR = S["PR"], S["DS"], S["DR"]

    def second_dot(r):
        v = jnp.dot(G[r, pl.ds(pl.multiple_of(oc * 128, 128), 128), :], W[...], preferred_element_type=F32)
        for i in range(16):
            DS[r, i, :, 0:Z] = v[:, i * Z : i * Z + Z].astype(BF16)
        cp = send(DS.at[r], DR.at[r], c=oc)
        v = jnp.dot(G[r, pl.ds(pl.multiple_of(c * 128, 128), 128), :], W[...], preferred_element_type=F32)
        for i in range(16):
            PR[r, i, :, 0:Z] = v[:, i * Z : i * Z + Z]
        return cp

    def place(order, yg, zg, xb):
        of = {"x": xb, "y": yg, "z": zg}
        return tuple(of[a] for a in order)

    def phase1(r, copy):
        copy.wait_recv()

        def part(i, _):
            yg, zg = i // 4, i % 4
            for xb in range(4):
                rows = pl.ds(xb * 32, 32)
                v = PR[r, i, rows, :] + DR[r, i, rows, :].astype(F32)
                PR[r, i, rows, :] = v
                for k, (order, tiles) in enumerate(COLOURS):
                    p, q, s = place(order, yg, zg, xb)
                    for t, (rb, lt) in enumerate(tiles[r]):
                        S[f"T1{r}{k}"][p, q * 4 + s, t] = v[rb * 8 : rb * 8 + 8, lt * 128 : lt * 128 + 128].astype(BF16)
            return 0

        lax.fori_loop(0, 16, part, 0)
        res = []
        for k, (order, _) in enumerate(COLOURS):
            a = order[0]
            T, R = S[f"T1{r}{k}"], S[f"R1{r}{k}"]
            res.append([send(T.at[step(a, d)], R.at[d - 1], **{a: step(a, d)}) for d in (1, 3, 2)])
        return res

    def phase2(r, copies):
        res = []
        for k, (order, tiles) in enumerate(COLOURS):
            for cp in copies[k]:
                cp.wait_recv()
            a, b, e = order
            R, T = S[f"R1{r}{k}"], S[f"T2{r}{k}"]

            def part(i, _, order=order, tiles=tiles[r], R=R, T=T):
                at = dict(zip(order, (co[order[0]], i // 4, i % 4)))
                for t, (rb, lt) in enumerate(tiles):
                    rows = pl.ds(pl.multiple_of(at["x"] * 32 + rb * 8, 8), 8)
                    v = PR[r, at["y"] * 4 + at["z"], rows, lt * 128 : lt * 128 + 128]
                    for d in range(3):
                        v = v + R[d, i, t].astype(F32)
                    T[i, t] = v.astype(BF16)
                return 0

            lax.fori_loop(0, 16, part, 0)
            R2 = S[f"R2{r}{k}"]
            res.append([
                send(T.at[step(b, d) * 4 + step(e, f)], R2.at[d * 4 + f - 1], **{b: step(b, d), e: step(e, f)})
                for d in range(4) for f in range(4) if d or f
            ])
        return res

    def finish(r, copies, weight):
        for k, (order, tiles) in enumerate(COLOURS):
            for cp in copies[k]:
                cp.wait_recv()
            _, b, e = order
            T2, R2 = S[f"T2{r}{k}"], S[f"R2{r}{k}"]
            for t, (rb, lt) in enumerate(tiles[r]):
                v = T2[co[b] * 4 + co[e], t].astype(F32)
                for j in range(15):
                    v = v + R2[j, t].astype(F32)
                lo, wide = r * 32 + rb * 8, min(128, Z - lt * 128)
                out[lo : lo + 8, lt * 128 : lt * 128 + wide] = weight[lo : lo + 8, :] * v[:, :wide]

    for d in (1, 3, 2):
        In[d] = send(IP.at[me], IP.at[me], x=step("x", d))
    Ic[0] = send(IP.at[me], IP.at[me], c=oc)
    send_x(0)
    send_x(1)
    tell(0)

    def pair(r, d):
        xs = step("x", 4 - d)
        sparse(r, c * 4 + xs)
        sparse(r, oc * 4 + xs)

    sparse(0, me)
    sparse(1, me)
    Ic[0].wait_recv()
    sparse(0, oc * 4 + x)
    sparse(1, oc * 4 + x)
    for d in (1, 3, 2):
        In[d].wait_recv()
        s = c * 4 + step("x", 4 - d)
        Ic[d] = send(IP.at[s], IP.at[s], c=oc)
    hear(0)
    tell(1)
    forward(0)
    for d in (1, 3, 2):
        Ic[d].wait_recv()
    pair(0, 1)
    forward(1)
    hear(1)
    tell(2)
    pair(0, 3)
    pair(0, 2)
    to_sibling(0)
    pair(1, 1)
    local[4].wait()
    for d in range(4):
        Cn[0][d].wait_recv()
    first_dot(0)
    to_sibling(1)
    a0 = stats(0)
    for d in range(4):
        Cn[1][d].wait_recv()
    first_dot(1)
    hear(2)
    b0 = second_stats(0, a0)
    a1 = stats(1)
    pair(1, 3)
    pair(1, 2)
    b1 = second_stats(1, a1)
    grads(0, b0)
    p0 = second_dot(0)
    p0 = phase1(0, p0)
    grads(1, b1)
    p1 = second_dot(1)
    p1 = phase1(1, p1)
    qa = spread(QA.at[me], True)
    p0 = phase2(0, p0)
    for cp in qa:
        cp.wait_recv()
    tot = QA[0]
    for k in range(1, 8):
        tot = tot + QA[k]
    QB[plane] = tot
    qb = spread(QB.at[plane], False)
    p1 = phase2(1, p1)

    local[5].wait()
    small = (
        lax.broadcasted_iota(jnp.int32, (64, 64), 0) == lax.broadcasted_iota(jnp.int32, (64, 64), 1)
    )
    weight = jnp.sum(jnp.where(small, jnp.broadcast_to(tw[...], (64, 64)), 0.0), axis=1, keepdims=True)
    for cp in qb:
        cp.wait_recv()
    tot = QB[0]
    for k in range(1, 16):
        tot = tot + QB[k]
    for r in range(2):
        for b in range(2):
            PK[b * 128 : b * 128 + 128, :] = to_col(tot[2 * r + b : 2 * r + b + 1, :])
        q = pr[r * 32 : r * 32 + 32, :]
        mass = jnp.sum(q, axis=1, keepdims=True)
        S["DV"][r * 32 : r * 32 + 32, :] = (
            jnp.sum(q * jnp.log(q), axis=1, keepdims=True) - PK[own, :] + mass * LN[r, own, :]
        )
    dv[...] = jnp.sum(jnp.where(small, jnp.broadcast_to(S["DV"][...], (64, 64)), 0.0), axis=0, keepdims=True)
    finish(0, p0, weight)
    finish(1, p1, weight)
    for cp in sent:
        cp.wait_send()


def hand_over(a, b, a_out, b_out):
    a_out[...] = a[...]
    b_out[...] = b[...]


def body(hidden, head_weight, teacher_ids, teacher_probs, token_weight):
    T, D = hidden.shape
    C = head_weight.shape[1]
    Z = D // 16
    V = pltpu.VMEM
    scratch = {
        "W": V((C, D), BF16), "H": V((2, 256, D), BF16), "IP": V((8, T, 128), F32),
        "SP": V((2, 256, C), F32), "L": V((2, 256, C), F32), "ST": V((256, 2), F32),
        "SA": V((2, 8, 8, 128), F32), "SB": V((2, 16, 8, 128), F32),
        "QA": V((8, 8, 128), F32), "QB": V((16, 8, 128), F32),
        "G": V((2, 256, C), BF16), "PK": V((256, 1), F32), "LN": V((2, 256, 1), F32),
        "DV": V((T, 1), F32),
        "PR": V((2, 16, 128, 256), F32), "DS": V((2, 16, 128, 256), BF16), "DR": V((2, 16, 128, 256), BF16),
        "ids": V(teacher_ids.shape, jnp.int32), "pr": V(teacher_probs.shape, F32), "tw": V((1, T), F32),
    }
    for r in range(2):
        for k, (_, tiles) in enumerate(COLOURS):
            n = len(tiles[r])
            scratch[f"T1{r}{k}"] = V((4, 16, n, 8, 128), BF16)
            scratch[f"R1{r}{k}"] = V((3, 16, n, 8, 128), BF16)
            scratch[f"T2{r}{k}"] = V((16, n, 8, 128), BF16)
            scratch[f"R2{r}{k}"] = V((15, n, 8, 128), BF16)
    scratch["ss"] = pltpu.SemaphoreType.DMA((260,))
    scratch["rs"] = pltpu.SemaphoreType.DMA((260,))
    scratch["hs"] = pltpu.SemaphoreType.REGULAR((3,))
    scratch["ls"] = pltpu.SemaphoreType.DMA((6,))
    vm = pl.BlockSpec(memory_space=pltpu.VMEM)
    grad, div = pl.pallas_call(
        functools.partial(kernel, names=tuple(scratch)),
        out_shape=(jax.ShapeDtypeStruct((T, Z), F32), jax.ShapeDtypeStruct((1, T), F32)),
        in_specs=[pl.BlockSpec(memory_space=pl.ANY)] * 5,
        out_specs=(vm, vm),
        scratch_shapes=list(scratch.values()),
        compiler_params=pltpu.CompilerParams(
            collective_id=0, has_side_effects=True, vmem_limit_bytes=67043328
        ),
        name="distill",
    )(hidden, head_weight.T, teacher_ids, teacher_probs, token_weight.reshape(1, T))
    grad, div = pl.pallas_call(
        hand_over,
        out_shape=(jax.ShapeDtypeStruct((T, Z), F32), jax.ShapeDtypeStruct((1, T), F32)),
        in_specs=[vm, vm],
        out_specs=(vm, vm),
        name="hand_over",
    )(grad, div)
    return div.reshape(T), grad


def solution(mesh):
    split = Mesh(mesh.devices.reshape(4, 2, 4, 4), ("x", "c", "y", "z"))
    placed = (P(DP, None), P(None, DP + VOCAB), P(DP, None), P(DP, None), P(DP))
    return jax.shard_map(
        body, mesh=split, in_specs=placed, out_specs=(P(DP), P(DP, VOCAB)), check_vma=False
    )
```

```python
import functools

import jax
import jax.numpy as jnp
from jax import lax
from jax.experimental import pallas as pl
from jax.experimental.pallas import tpu as pltpu
from jax.sharding import Mesh
from jax.sharding import PartitionSpec as P

MESH = pl.DeviceIdType.MESH
DP = ("x", "c")
VOCAB = ("y", "z")
F32 = jnp.float32
BF16 = jnp.bfloat16
COLOURS = (
    (("x", "y", "z"), (((0, 0), (0, 1), (3, 0)), ((0, 0), (0, 1)))),
    (("y", "z", "x"), (((1, 0), (1, 1), (3, 1)), ((1, 0), (1, 1), (3, 0)))),
    (("z", "x", "y"), (((2, 0), (2, 1)), ((2, 0), (2, 1), (3, 1)))),
)


FAR_FIRST = sorted(((d, e) for d in range(4) for e in range(4) if d or e), key=lambda p: -sum(min(v, 4 - v) for v in p))


def kernel(h, w, ids_in, pr_in, tw_in, out, dv, *scratch, names):
    S = dict(zip(names, scratch))
    D = h.shape[1]
    C = w.shape[0]
    TOP = ids_in.shape[1]
    Z = D // 16
    co = {a: lax.axis_index(a) for a in ("x", "c", "y", "z")}
    x, c, y, z = co["x"], co["c"], co["y"], co["z"]
    oc = 1 - c
    count = [0]

    def step(axis, d):
        return lax.rem(co[axis] + d, 4)

    def send(src, dst, **dev):
        i = count[0]
        count[0] += 1
        cp = pltpu.make_async_remote_copy(
            src_ref=src, dst_ref=dst, send_sem=S["ss"].at[i], recv_sem=S["rs"].at[i],
            device_id=dev, device_id_type=MESH,
        )
        cp.start()
        sent.append(cp)
        return cp

    sent = []
    bar = pltpu.get_barrier_semaphore()
    for d in range(4):
        for e in range(2):
            if d or e:
                pl.semaphore_signal(
                    bar, inc=1, device_id={"x": step("x", d), "c": lax.rem(c + e, 2)}, device_id_type=MESH
                )
    beside = [{"y": step("y", 1)}, {"y": step("y", 3)}, {"z": step("z", 1)}, {"z": step("z", 3)}]
    for dev in beside:
        pl.semaphore_signal(bar, inc=1, device_id=dev, device_id_type=MESH)
    H, IP, W = S["H"], S["IP"], S["W"]
    me = c * 4 + x
    own = pl.ds(pl.multiple_of(me * 32, 32), 32)
    ids, pr, tw = S["ids"], S["pr"], S["tw"]
    local = [
        pltpu.make_async_copy(ids_in, ids, S["ls"].at[0]),
        pltpu.make_async_copy(pr_in, pr, S["ls"].at[1]),
        pltpu.make_async_copy(h.at[0:32, :], H.at[0, own, :], S["ls"].at[2]),
        pltpu.make_async_copy(h.at[32:64, :], H.at[1, own, :], S["ls"].at[3]),
        pltpu.make_async_copy(w, W, S["ls"].at[4]),
        pltpu.make_async_copy(tw_in, tw, S["ls"].at[5]),
    ]
    for cp in local:
        cp.start()
    for cp in local[:2]:
        cp.wait()
    IP[me, :, 0:TOP] = pr[...]
    IP[me, :, TOP : 2 * TOP] = ids[...].astype(F32)
    for cp in local[2:4]:
        cp.wait()
    pl.semaphore_wait(bar, 11)

    def tell(i):
        for dev in beside:
            pl.semaphore_signal(S["hs"].at[i], inc=1, device_id=dev, device_id_type=MESH)

    def hear(i):
        pl.semaphore_wait(S["hs"].at[i], 4)

    share = (lax.rem(y + 2 * z, 4), lax.rem(2 * y + z, 4))
    X, Pn, Cn, In, Ic = [{}, {}], [{}, {}], [{}, {}], {}, {}

    def hrows(r, core, xb, off, n):
        return H.at[r, pl.ds(pl.multiple_of(core * 128 + xb * 32 + off, 8), n), :]

    def send_x(r):
        for d in (1, 3, 2):
            X[r][d] = []
            for half in range(2):
                rows = pl.ds(pl.multiple_of(me * 32 + share[half] * 8, 8), 8)
                part = H.at[r, rows, half * (D // 2) : (half + 1) * (D // 2)]
                X[r][d].append(send(part, part, x=step("x", d)))
        whole = hrows(r, c, x, 0, 32)
        Cn[r][0] = send(whole, whole, c=oc)

    def forward(r):
        for d in (1, 3, 2):
            xs = step("x", 4 - d)
            Pn[r][d] = []
            for half in range(2):
                X[r][d][half].wait_recv()
                more, less = (("y", "z"), ("z", "y"))[half]
                rows = pl.ds(pl.multiple_of(c * 128 + xs * 32 + share[half] * 8, 8), 8)
                at = half * (D // 2)
                whole = H.at[r, rows, at : at + D // 2]
                lo, hi = H.at[r, rows, at : at + D // 4], H.at[r, rows, at + D // 4 : at + D // 2]
                Pn[r][d] += [
                    send(whole, whole, **{more: step(more, 1)}),
                    send(whole, whole, **{more: step(more, 3)}),
                    send(lo, lo, **{less: step(less, 1)}),
                    send(hi, hi, **{less: step(less, 3)}),
                ]

    def to_sibling(r):
        for d in (1, 3, 2):
            for cp in Pn[r][d]:
                cp.wait_recv()
            xs = step("x", 4 - d)
            blk = hrows(r, c, xs, 0, 32)
            Cn[r][d] = send(blk, blk, c=oc)

    dp_index = x * 2 + c
    offset = (dp_index * 16 + y * 4 + z) * C
    SP = S["SP"]

    def sparse(r, blk):
        def group(i, _):
            g = blk * 2 + i
            j0 = r * 32 + i * 16
            rows = pl.ds(pl.multiple_of(j0, 16), 16)
            local = IP[blk, rows, TOP : 2 * TOP].astype(jnp.int32) - offset
            local = jnp.where((local >= 0) & (local < C), local, -1).astype(jnp.int16)
            lane = lax.broadcasted_iota(jnp.int32, (16, 128), 1)
            n = -(-C // 128)
            cols = [(lane + 128 * k).astype(jnp.int16) for k in range(n)]
            acc = [jnp.full((16, 128), 127, jnp.int16) for _ in range(n)]
            for k in range(TOP):
                one = jnp.broadcast_to(local[:, k : k + 1], (16, 128))
                for j in range(n):
                    acc[j] = jnp.where(one == cols[j], jnp.int16(k), acc[j])
            for j in range(n):
                which = acc[j].astype(jnp.int32)
                wide = min(128, C - 128 * j)
                for s in range(2):
                    table = IP[blk, pl.ds(pl.multiple_of(j0 + s * 8, 8), 8), :]
                    sel = which[s * 8 : s * 8 + 8]
                    got = jnp.where(sel < TOP, jnp.take_along_axis(table, sel, axis=1), 0.0)
                    SP[r, pl.ds(pl.multiple_of(g * 16 + s * 8, 8), 8), 128 * j : 128 * j + wide] = got[:, :wide]
            return 0

        lax.fori_loop(0, 2, group, 0)

    eye = (
        lax.broadcasted_iota(jnp.int32, (128, 128), 0) == lax.broadcasted_iota(jnp.int32, (128, 128), 1)
    )

    def to_row(col):
        return jnp.sum(jnp.where(eye, jnp.broadcast_to(col, (128, 128)), 0.0), axis=0, keepdims=True)

    def to_col(row):
        return jnp.sum(jnp.where(eye, jnp.broadcast_to(row, (128, 128)), 0.0), axis=1, keepdims=True)

    L, ST = S["L"], S["ST"]
    SA, SB = S["SA"], S["SB"]

    def spread(ref, near):
        if near:
            return [
                send(ref, ref, x=step("x", d), c=lax.rem(c + e, 2))
                for d in (2, 1, 3, 0) for e in range(2) if d or e
            ]
        return [
            send(ref, ref, y=step("y", d), z=step("z", e))
            for d, e in FAR_FIRST
        ]

    def first_dot(r):
        L[r] = lax.dot_general(
            H[r], W[...], (((1,), (1,)), ((), ())), preferred_element_type=F32
        )

    def stats(r):
        def part(i, _):
            rows = pl.ds(pl.multiple_of(i * 32, 32), 32)
            v = L[r, rows, :]
            m = jnp.max(v, axis=1, keepdims=True)
            ST[rows, 0:1] = m
            ST[rows, 1:2] = jnp.sum(jnp.exp(v - m), axis=1, keepdims=True)
            return 0

        lax.fori_loop(0, 8, part, 0)
        for b in range(2):
            SA[r, me, b : b + 1, :] = to_row(ST[b * 128 : b * 128 + 128, 0:1])
            SA[r, me, b + 2 : b + 3, :] = to_row(ST[b * 128 : b * 128 + 128, 1:2])
        return spread(SA.at[r, me], True)

    def merged(buf, r, n, copies):
        for cp in copies:
            cp.wait_recv()
        m = buf[r, 0, 0:2, :]
        for k in range(1, n):
            m = jnp.maximum(m, buf[r, k, 0:2, :])
        s = jnp.zeros_like(m)
        for k in range(n):
            s = s + buf[r, k, 2:4, :] * jnp.exp(buf[r, k, 0:2, :] - m)
        return m, s

    plane = y * 4 + z

    def second_stats(r, copies):
        m, s = merged(SA, r, 8, copies)
        SB[r, plane, 0:2, :] = m
        SB[r, plane, 2:4, :] = s
        return spread(SB.at[r, plane], False)

    G, PK, LN, QA, QB = S["G"], S["PK"], S["LN"], S["QA"], S["QB"]

    def grads(r, copies):
        m, s = merged(SB, r, 16, copies)
        norm = m + jnp.log(s)
        for b in range(2):
            LN[r, b * 128 : b * 128 + 128, :] = to_col(norm[b : b + 1, :])

        def part(i, _):
            rows = pl.ds(pl.multiple_of(i * 32, 32), 32)
            v = L[r, rows, :]
            sp = SP[r, rows, :]
            mass = jnp.sum(IP[i, r * 32 : r * 32 + 32, 0:TOP], axis=1, keepdims=True)
            G[r, rows, :] = (mass * jnp.exp(v - LN[r, rows, :]) - sp).astype(BF16)
            PK[rows, :] = jnp.sum(sp * v, axis=1, keepdims=True)
            return 0

        lax.fori_loop(0, 8, part, 0)
        for b in range(2):
            QA[me, 2 * r + b : 2 * r + b + 1, :] = to_row(PK[b * 128 : b * 128 + 128, :])

    PR, DS, DR = S["PR"], S["DS"], S["DR"]

    def second_dot(r):
        v = jnp.dot(G[r, pl.ds(pl.multiple_of(oc * 128, 128), 128), :], W[...], preferred_element_type=F32)
        for i in range(16):
            DS[r, i, :, 0:Z] = v[:, i * Z : i * Z + Z].astype(BF16)
        cp = send(DS.at[r], DR.at[r], c=oc)
        v = jnp.dot(G[r, pl.ds(pl.multiple_of(c * 128, 128), 128), :], W[...], preferred_element_type=F32)
        for i in range(16):
            PR[r, i, :, 0:Z] = v[:, i * Z : i * Z + Z]
        return cp

    def place(order, yg, zg, xb):
        of = {"x": xb, "y": yg, "z": zg}
        return tuple(of[a] for a in order)

    def phase1(r, copy):
        copy.wait_recv()

        def part(i, _):
            yg, zg = i // 4, i % 4
            for xb in range(4):
                rows = pl.ds(xb * 32, 32)
                v = PR[r, i, rows, :] + DR[r, i, rows, :].astype(F32)
                PR[r, i, rows, :] = v
                for k, (order, tiles) in enumerate(COLOURS):
                    p, q, s = place(order, yg, zg, xb)
                    for t, (rb, lt) in enumerate(tiles[r]):
                        S[f"T1{r}{k}"][p, q * 4 + s, t] = v[rb * 8 : rb * 8 + 8, lt * 128 : lt * 128 + 128].astype(BF16)
            return 0

        lax.fori_loop(0, 16, part, 0)
        res = []
        for k, (order, _) in enumerate(COLOURS):
            a = order[0]
            T, R = S[f"T1{r}{k}"], S[f"R1{r}{k}"]
            res.append([send(T.at[step(a, d)], R.at[d - 1], **{a: step(a, d)}) for d in (2, 1, 3)])
        return res

    def phase2(r, copies):
        res = []
        for k, (order, tiles) in enumerate(COLOURS):
            for cp in copies[k]:
                cp.wait_recv()
            a, b, e = order
            R, T = S[f"R1{r}{k}"], S[f"T2{r}{k}"]

            def part(i, _, order=order, tiles=tiles[r], R=R, T=T):
                at = dict(zip(order, (co[order[0]], i // 4, i % 4)))
                for t, (rb, lt) in enumerate(tiles):
                    rows = pl.ds(pl.multiple_of(at["x"] * 32 + rb * 8, 8), 8)
                    v = PR[r, at["y"] * 4 + at["z"], rows, lt * 128 : lt * 128 + 128]
                    for d in range(3):
                        v = v + R[d, i, t].astype(F32)
                    T[i, t] = v.astype(BF16)
                return 0

            lax.fori_loop(0, 16, part, 0)
            R2 = S[f"R2{r}{k}"]
            res.append([
                send(T.at[step(b, d) * 4 + step(e, f)], R2.at[d * 4 + f - 1], **{b: step(b, d), e: step(e, f)})
                for d, f in FAR_FIRST
            ])
        return res

    def finish(r, copies, weight):
        for k, (order, tiles) in enumerate(COLOURS):
            for cp in copies[k]:
                cp.wait_recv()
            _, b, e = order
            T2, R2 = S[f"T2{r}{k}"], S[f"R2{r}{k}"]
            for t, (rb, lt) in enumerate(tiles[r]):
                v = T2[co[b] * 4 + co[e], t].astype(F32)
                for j in range(15):
                    v = v + R2[j, t].astype(F32)
                lo, wide = r * 32 + rb * 8, min(128, Z - lt * 128)
                out[lo : lo + 8, lt * 128 : lt * 128 + wide] = weight[lo : lo + 8, :] * v[:, :wide]

    for d in (1, 3, 2):
        In[d] = send(IP.at[me], IP.at[me], x=step("x", d))
    Ic[0] = send(IP.at[me], IP.at[me], c=oc)
    send_x(0)
    send_x(1)
    tell(0)

    def pair(r, d):
        xs = step("x", 4 - d)
        sparse(r, c * 4 + xs)
        sparse(r, oc * 4 + xs)

    sparse(0, me)
    sparse(1, me)
    Ic[0].wait_recv()
    sparse(0, oc * 4 + x)
    sparse(1, oc * 4 + x)
    for d in (1, 3, 2):
        In[d].wait_recv()
        s = c * 4 + step("x", 4 - d)
        Ic[d] = send(IP.at[s], IP.at[s], c=oc)
    hear(0)
    tell(1)
    forward(0)
    for d in (1, 3, 2):
        Ic[d].wait_recv()
    pair(0, 1)
    forward(1)
    hear(1)
    tell(2)
    pair(0, 3)
    pair(0, 2)
    to_sibling(0)
    pair(1, 1)
    local[4].wait()
    for d in range(4):
        Cn[0][d].wait_recv()
    first_dot(0)
    to_sibling(1)
    a0 = stats(0)
    for d in range(4):
        Cn[1][d].wait_recv()
    first_dot(1)
    hear(2)
    b0 = second_stats(0, a0)
    a1 = stats(1)
    pair(1, 3)
    pair(1, 2)
    b1 = second_stats(1, a1)
    grads(0, b0)
    p0 = second_dot(0)
    p0 = phase1(0, p0)
    grads(1, b1)
    p1 = second_dot(1)
    p1 = phase1(1, p1)
    qa = spread(QA.at[me], True)
    p0 = phase2(0, p0)
    for cp in qa:
        cp.wait_recv()
    tot = QA[0]
    for k in range(1, 8):
        tot = tot + QA[k]
    QB[plane] = tot
    qb = spread(QB.at[plane], False)
    p1 = phase2(1, p1)

    local[5].wait()
    small = (
        lax.broadcasted_iota(jnp.int32, (64, 64), 0) == lax.broadcasted_iota(jnp.int32, (64, 64), 1)
    )
    weight = jnp.sum(jnp.where(small, jnp.broadcast_to(tw[...], (64, 64)), 0.0), axis=1, keepdims=True)
    for cp in qb:
        cp.wait_recv()
    tot = QB[0]
    for k in range(1, 16):
        tot = tot + QB[k]
    for r in range(2):
        for b in range(2):
            PK[b * 128 : b * 128 + 128, :] = to_col(tot[2 * r + b : 2 * r + b + 1, :])
        q = pr[r * 32 : r * 32 + 32, :]
        mass = jnp.sum(q, axis=1, keepdims=True)
        S["DV"][r * 32 : r * 32 + 32, :] = (
            jnp.sum(q * jnp.log(q), axis=1, keepdims=True) - PK[own, :] + mass * LN[r, own, :]
        )
    dv[...] = jnp.sum(jnp.where(small, jnp.broadcast_to(S["DV"][...], (64, 64)), 0.0), axis=0, keepdims=True)
    finish(0, p0, weight)
    finish(1, p1, weight)
    for cp in sent:
        cp.wait_send()


def hand_over(a, b, a_out, b_out):
    a_out[...] = a[...]
    b_out[...] = b[...]


def body(hidden, head_weight, teacher_ids, teacher_probs, token_weight):
    T, D = hidden.shape
    C = head_weight.shape[1]
    Z = D // 16
    V = pltpu.VMEM
    scratch = {
        "W": V((C, D), BF16), "H": V((2, 256, D), BF16), "IP": V((8, T, 128), F32),
        "SP": V((2, 256, C), F32), "L": V((2, 256, C), F32), "ST": V((256, 2), F32),
        "SA": V((2, 8, 8, 128), F32), "SB": V((2, 16, 8, 128), F32),
        "QA": V((8, 8, 128), F32), "QB": V((16, 8, 128), F32),
        "G": V((2, 256, C), BF16), "PK": V((256, 1), F32), "LN": V((2, 256, 1), F32),
        "DV": V((T, 1), F32),
        "PR": V((2, 16, 128, 256), F32), "DS": V((2, 16, 128, 256), BF16), "DR": V((2, 16, 128, 256), BF16),
        "ids": V(teacher_ids.shape, jnp.int32), "pr": V(teacher_probs.shape, F32), "tw": V((1, T), F32),
    }
    for r in range(2):
        for k, (_, tiles) in enumerate(COLOURS):
            n = len(tiles[r])
            scratch[f"T1{r}{k}"] = V((4, 16, n, 8, 128), BF16)
            scratch[f"R1{r}{k}"] = V((3, 16, n, 8, 128), BF16)
            scratch[f"T2{r}{k}"] = V((16, n, 8, 128), BF16)
            scratch[f"R2{r}{k}"] = V((15, n, 8, 128), BF16)
    scratch["ss"] = pltpu.SemaphoreType.DMA((260,))
    scratch["rs"] = pltpu.SemaphoreType.DMA((260,))
    scratch["hs"] = pltpu.SemaphoreType.REGULAR((3,))
    scratch["ls"] = pltpu.SemaphoreType.DMA((6,))
    vm = pl.BlockSpec(memory_space=pltpu.VMEM)
    grad, div = pl.pallas_call(
        functools.partial(kernel, names=tuple(scratch)),
        out_shape=(jax.ShapeDtypeStruct((T, Z), F32), jax.ShapeDtypeStruct((1, T), F32)),
        in_specs=[pl.BlockSpec(memory_space=pl.ANY)] * 5,
        out_specs=(vm, vm),
        scratch_shapes=list(scratch.values()),
        compiler_params=pltpu.CompilerParams(
            collective_id=0, has_side_effects=True, vmem_limit_bytes=67043328
        ),
        name="distill",
    )(hidden, head_weight.T, teacher_ids, teacher_probs, token_weight.reshape(1, T))
    grad, div = pl.pallas_call(
        hand_over,
        out_shape=(jax.ShapeDtypeStruct((T, Z), F32), jax.ShapeDtypeStruct((1, T), F32)),
        in_specs=[vm, vm],
        out_specs=(vm, vm),
        name="hand_over",
    )(grad, div)
    return div.reshape(T), grad


def solution(mesh):
    split = Mesh(mesh.devices.reshape(4, 2, 4, 4), ("x", "c", "y", "z"))
    placed = (P(DP, None), P(None, DP + VOCAB), P(DP, None), P(DP, None), P(DP))
    return jax.shard_map(
        body, mesh=split, in_specs=placed, out_specs=(P(DP), P(DP, VOCAB)), check_vma=False
    )
```

```python
import functools

import jax
import jax.numpy as jnp
from jax import lax
from jax.experimental import pallas as pl
from jax.experimental.pallas import tpu as pltpu
from jax.sharding import Mesh
from jax.sharding import PartitionSpec as P

MESH = pl.DeviceIdType.MESH
DP = ("x", "c")
VOCAB = ("y", "z")
F32 = jnp.float32
BF16 = jnp.bfloat16
COLOURS = (
    (("x", "y", "z"), (((0, 0), (0, 1), (3, 0)), ((0, 0), (0, 1)))),
    (("y", "z", "x"), (((1, 0), (1, 1), (3, 1)), ((1, 0), (1, 1), (3, 0)))),
    (("z", "x", "y"), (((2, 0), (2, 1)), ((2, 0), (2, 1), (3, 1)))),
)


FAR_FIRST = sorted(((d, e) for d in range(4) for e in range(4) if d or e), key=lambda p: -sum(min(v, 4 - v) for v in p))


def kernel(h, w, ids_in, pr_in, tw_in, out, dv, *scratch, names):
    S = dict(zip(names, scratch))
    D = h.shape[1]
    C = w.shape[0]
    TOP = ids_in.shape[1]
    Z = D // 16
    co = {a: lax.axis_index(a) for a in ("x", "c", "y", "z")}
    x, c, y, z = co["x"], co["c"], co["y"], co["z"]
    oc = 1 - c
    count = [0]

    def step(axis, d):
        return lax.rem(co[axis] + d, 4)

    def send(src, dst, **dev):
        i = count[0]
        count[0] += 1
        cp = pltpu.make_async_remote_copy(
            src_ref=src, dst_ref=dst, send_sem=S["ss"].at[i], recv_sem=S["rs"].at[i],
            device_id=dev, device_id_type=MESH,
        )
        cp.start()
        sent.append(cp)
        return cp

    sent = []
    bar = pltpu.get_barrier_semaphore()
    for d in range(4):
        for e in range(2):
            if d or e:
                pl.semaphore_signal(
                    bar, inc=1, device_id={"x": step("x", d), "c": lax.rem(c + e, 2)}, device_id_type=MESH
                )
    beside = [{"y": step("y", 1)}, {"y": step("y", 3)}, {"z": step("z", 1)}, {"z": step("z", 3)}]
    for dev in beside:
        pl.semaphore_signal(bar, inc=1, device_id=dev, device_id_type=MESH)
    H, IP, W = S["H"], S["IP"], S["W"]
    me = c * 4 + x
    own = pl.ds(pl.multiple_of(me * 32, 32), 32)
    ids, pr, tw = S["ids"], S["pr"], S["tw"]
    local = [
        pltpu.make_async_copy(ids_in, ids, S["ls"].at[0]),
        pltpu.make_async_copy(pr_in, pr, S["ls"].at[1]),
        pltpu.make_async_copy(h.at[0:32, :], H.at[0, own, :], S["ls"].at[2]),
        pltpu.make_async_copy(h.at[32:64, :], H.at[1, own, :], S["ls"].at[3]),
        pltpu.make_async_copy(w, W, S["ls"].at[4]),
        pltpu.make_async_copy(tw_in, tw, S["ls"].at[5]),
    ]
    for cp in local:
        cp.start()
    for cp in local[:2]:
        cp.wait()
    IP[me, :, 0:TOP] = pr[...]
    IP[me, :, TOP : 2 * TOP] = ids[...].astype(F32)
    for cp in local[2:4]:
        cp.wait()
    pl.semaphore_wait(bar, 11)

    def tell(i):
        for dev in beside:
            pl.semaphore_signal(S["hs"].at[i], inc=1, device_id=dev, device_id_type=MESH)

    def hear(i):
        pl.semaphore_wait(S["hs"].at[i], 4)

    share = (lax.rem(y + 2 * z, 4), lax.rem(2 * y + z, 4))
    X, Pn, Cn, In, Ic = [{}, {}], [{}, {}], [{}, {}], {}, {}

    def hrows(r, core, xb, off, n):
        return H.at[r, pl.ds(pl.multiple_of(core * 128 + xb * 32 + off, 8), n), :]

    def send_x(r):
        for d in (1, 3, 2):
            X[r][d] = []
            for half in range(2):
                rows = pl.ds(pl.multiple_of(me * 32 + share[half] * 8, 8), 8)
                part = H.at[r, rows, half * (D // 2) : (half + 1) * (D // 2)]
                X[r][d].append(send(part, part, x=step("x", d)))
        whole = hrows(r, c, x, 0, 32)
        Cn[r][0] = send(whole, whole, c=oc)

    def forward(r):
        for d in (1, 3, 2):
            xs = step("x", 4 - d)
            Pn[r][d] = []
            for half in range(2):
                X[r][d][half].wait_recv()
                more, less = (("y", "z"), ("z", "y"))[half]
                rows = pl.ds(pl.multiple_of(c * 128 + xs * 32 + share[half] * 8, 8), 8)
                at = half * (D // 2)
                whole = H.at[r, rows, at : at + D // 2]
                lo, hi = H.at[r, rows, at : at + D // 4], H.at[r, rows, at + D // 4 : at + D // 2]
                Pn[r][d] += [
                    send(whole, whole, **{more: step(more, 1)}),
                    send(whole, whole, **{more: step(more, 3)}),
                    send(lo, lo, **{less: step(less, 1)}),
                    send(hi, hi, **{less: step(less, 3)}),
                ]

    def to_sibling(r):
        for d in (1, 3, 2):
            for cp in Pn[r][d]:
                cp.wait_recv()
            xs = step("x", 4 - d)
            blk = hrows(r, c, xs, 0, 32)
            Cn[r][d] = send(blk, blk, c=oc)

    dp_index = x * 2 + c
    offset = (dp_index * 16 + y * 4 + z) * C
    SP = S["SP"]

    def sparse(r, blk):
        def group(i, _):
            g = blk * 2 + i
            j0 = r * 32 + i * 16
            rows = pl.ds(pl.multiple_of(j0, 16), 16)
            local = IP[blk, rows, TOP : 2 * TOP].astype(jnp.int32) - offset
            local = jnp.where((local >= 0) & (local < C), local, -1).astype(jnp.int16)
            lane = lax.broadcasted_iota(jnp.int32, (16, 128), 1)
            n = -(-C // 128)
            cols = [(lane + 128 * k).astype(jnp.int16) for k in range(n)]
            acc = [jnp.full((16, 128), 127, jnp.int16) for _ in range(n)]
            for k in range(TOP):
                one = jnp.broadcast_to(local[:, k : k + 1], (16, 128))
                for j in range(n):
                    acc[j] = jnp.where(one == cols[j], jnp.int16(k), acc[j])
            for j in range(n):
                which = acc[j].astype(jnp.int32)
                wide = min(128, C - 128 * j)
                for s in range(2):
                    table = IP[blk, pl.ds(pl.multiple_of(j0 + s * 8, 8), 8), :]
                    sel = which[s * 8 : s * 8 + 8]
                    got = jnp.where(sel < TOP, jnp.take_along_axis(table, sel, axis=1), 0.0)
                    SP[r, pl.ds(pl.multiple_of(g * 16 + s * 8, 8), 8), 128 * j : 128 * j + wide] = got[:, :wide]
            return 0

        lax.fori_loop(0, 2, group, 0)

    eye = (
        lax.broadcasted_iota(jnp.int32, (128, 128), 0) == lax.broadcasted_iota(jnp.int32, (128, 128), 1)
    )

    def to_row(col):
        return jnp.sum(jnp.where(eye, jnp.broadcast_to(col, (128, 128)), 0.0), axis=0, keepdims=True)

    def to_col(row):
        return jnp.sum(jnp.where(eye, jnp.broadcast_to(row, (128, 128)), 0.0), axis=1, keepdims=True)

    L, ST = S["L"], S["ST"]
    SA, SB = S["SA"], S["SB"]

    def spread(ref, near):
        if near:
            return [
                send(ref, ref, x=step("x", d), c=lax.rem(c + e, 2))
                for d in (2, 1, 3, 0) for e in range(2) if d or e
            ]
        return [
            send(ref, ref, y=step("y", d), z=step("z", e))
            for d, e in FAR_FIRST
        ]

    def first_dot(r):
        L[r] = lax.dot_general(
            H[r], W[...], (((1,), (1,)), ((), ())), preferred_element_type=F32
        )

    def stats(r):
        def part(i, _):
            rows = pl.ds(pl.multiple_of(i * 32, 32), 32)
            v = L[r, rows, :]
            m = jnp.max(v, axis=1, keepdims=True)
            ST[rows, 0:1] = m
            ST[rows, 1:2] = jnp.sum(jnp.exp(v - m), axis=1, keepdims=True)
            return 0

        lax.fori_loop(0, 8, part, 0)
        for b in range(2):
            SA[r, me, b : b + 1, :] = to_row(ST[b * 128 : b * 128 + 128, 0:1])
            SA[r, me, b + 2 : b + 3, :] = to_row(ST[b * 128 : b * 128 + 128, 1:2])
        return spread(SA.at[r, me], True)

    def merged(buf, r, n, copies):
        for cp in copies:
            cp.wait_recv()
        m = buf[r, 0, 0:2, :]
        for k in range(1, n):
            m = jnp.maximum(m, buf[r, k, 0:2, :])
        s = jnp.zeros_like(m)
        for k in range(n):
            s = s + buf[r, k, 2:4, :] * jnp.exp(buf[r, k, 0:2, :] - m)
        return m, s

    plane = y * 4 + z

    def second_stats(r, copies):
        m, s = merged(SA, r, 8, copies)
        SB[r, plane, 0:2, :] = m
        SB[r, plane, 2:4, :] = s
        return spread(SB.at[r, plane], False)

    G, PK, LN, QA, QB = S["G"], S["PK"], S["LN"], S["QA"], S["QB"]

    def grads(r, copies):
        m, s = merged(SB, r, 16, copies)
        norm = m + jnp.log(s)
        for b in range(2):
            LN[r, b * 128 : b * 128 + 128, :] = to_col(norm[b : b + 1, :])

        def part(i, _):
            rows = pl.ds(pl.multiple_of(i * 32, 32), 32)
            v = L[r, rows, :]
            sp = SP[r, rows, :]
            mass = jnp.sum(IP[i, r * 32 : r * 32 + 32, 0:TOP], axis=1, keepdims=True)
            G[r, rows, :] = (mass * jnp.exp(v - LN[r, rows, :]) - sp).astype(BF16)
            PK[rows, :] = jnp.sum(sp * v, axis=1, keepdims=True)
            return 0

        lax.fori_loop(0, 8, part, 0)
        for b in range(2):
            QA[me, 2 * r + b : 2 * r + b + 1, :] = to_row(PK[b * 128 : b * 128 + 128, :])

    PR, DS, DR = S["PR"], S["DS"], S["DR"]

    def second_dot(r):
        v = jnp.dot(G[r, pl.ds(pl.multiple_of(oc * 128, 128), 128), :], W[...], preferred_element_type=F32)
        for i in range(16):
            DS[r, i, :, 0:Z] = v[:, i * Z : i * Z + Z].astype(BF16)
        cp = send(DS.at[r], DR.at[r], c=oc)
        v = jnp.dot(G[r, pl.ds(pl.multiple_of(c * 128, 128), 128), :], W[...], preferred_element_type=F32)
        for i in range(16):
            PR[r, i, :, 0:Z] = v[:, i * Z : i * Z + Z]
        return cp

    def place(order, yg, zg, xb):
        of = {"x": xb, "y": yg, "z": zg}
        return tuple(of[a] for a in order)

    def phase1(r, copy):
        copy.wait_recv()

        def part(i, _):
            yg, zg = i // 4, i % 4
            for xb in range(4):
                rows = pl.ds(xb * 32, 32)
                v = PR[r, i, rows, :] + DR[r, i, rows, :].astype(F32)
                PR[r, i, rows, :] = v
                for k, (order, tiles) in enumerate(COLOURS):
                    p, q, s = place(order, yg, zg, xb)
                    for t, (rb, lt) in enumerate(tiles[r]):
                        S[f"T1{r}{k}"][p, q * 4 + s, t] = v[rb * 8 : rb * 8 + 8, lt * 128 : lt * 128 + 128].astype(BF16)
            return 0

        lax.fori_loop(0, 16, part, 0)
        res = []
        for k, (order, _) in enumerate(COLOURS):
            a = order[0]
            T, R = S[f"T1{r}{k}"], S[f"R1{r}{k}"]
            res.append([send(T.at[step(a, d)], R.at[d - 1], **{a: step(a, d)}) for d in (2, 1, 3)])
        return res

    def phase2(r, copies):
        res = []
        for k, (order, tiles) in enumerate(COLOURS):
            for cp in copies[k]:
                cp.wait_recv()
            a, b, e = order
            R, T = S[f"R1{r}{k}"], S[f"T2{r}{k}"]

            def part(i, _, order=order, tiles=tiles[r], R=R, T=T):
                at = dict(zip(order, (co[order[0]], i // 4, i % 4)))
                for t, (rb, lt) in enumerate(tiles):
                    rows = pl.ds(pl.multiple_of(at["x"] * 32 + rb * 8, 8), 8)
                    v = PR[r, at["y"] * 4 + at["z"], rows, lt * 128 : lt * 128 + 128]
                    for d in range(3):
                        v = v + R[d, i, t].astype(F32)
                    T[i, t] = v.astype(BF16)
                return 0

            lax.fori_loop(0, 16, part, 0)
            R2 = S[f"R2{r}{k}"]
            res.append([
                send(T.at[step(b, d) * 4 + step(e, f)], R2.at[d * 4 + f - 1], **{b: step(b, d), e: step(e, f)})
                for d, f in FAR_FIRST
            ])
        return res

    def finish(r, copies, weight):
        for k, (order, tiles) in enumerate(COLOURS):
            for cp in copies[k]:
                cp.wait_recv()
            _, b, e = order
            T2, R2 = S[f"T2{r}{k}"], S[f"R2{r}{k}"]
            for t, (rb, lt) in enumerate(tiles[r]):
                v = T2[co[b] * 4 + co[e], t].astype(F32)
                for j in range(15):
                    v = v + R2[j, t].astype(F32)
                lo, wide = r * 32 + rb * 8, min(128, Z - lt * 128)
                out[lo : lo + 8, lt * 128 : lt * 128 + wide] = weight[lo : lo + 8, :] * v[:, :wide]

    for d in (1, 3, 2):
        In[d] = send(IP.at[me], IP.at[me], x=step("x", d))
    Ic[0] = send(IP.at[me], IP.at[me], c=oc)
    send_x(0)
    send_x(1)
    tell(0)

    def pair(r, d):
        xs = step("x", 4 - d)
        sparse(r, c * 4 + xs)
        sparse(r, oc * 4 + xs)

    sparse(0, me)
    sparse(1, me)
    Ic[0].wait_recv()
    sparse(0, oc * 4 + x)
    sparse(1, oc * 4 + x)
    for d in (1, 3, 2):
        In[d].wait_recv()
        s = c * 4 + step("x", 4 - d)
        Ic[d] = send(IP.at[s], IP.at[s], c=oc)
    hear(0)
    tell(1)
    forward(0)
    for d in (1, 3, 2):
        Ic[d].wait_recv()
    pair(0, 1)
    forward(1)
    hear(1)
    tell(2)
    pair(0, 3)
    pair(0, 2)
    to_sibling(0)
    pair(1, 1)
    local[4].wait()
    for d in range(4):
        Cn[0][d].wait_recv()
    first_dot(0)
    to_sibling(1)
    a0 = stats(0)
    for d in range(4):
        Cn[1][d].wait_recv()
    first_dot(1)
    hear(2)
    b0 = second_stats(0, a0)
    a1 = stats(1)
    pair(1, 3)
    pair(1, 2)
    b1 = second_stats(1, a1)
    grads(0, b0)
    p0 = second_dot(0)
    p0 = phase1(0, p0)
    grads(1, b1)
    p1 = second_dot(1)
    p1 = phase1(1, p1)
    qa = spread(QA.at[me], True)
    p0 = phase2(0, p0)
    for cp in qa:
        cp.wait_recv()
    tot = QA[0]
    for k in range(1, 8):
        tot = tot + QA[k]
    QB[plane] = tot
    qb = spread(QB.at[plane], False)
    p1 = phase2(1, p1)

    local[5].wait()
    small = (
        lax.broadcasted_iota(jnp.int32, (64, 64), 0) == lax.broadcasted_iota(jnp.int32, (64, 64), 1)
    )
    weight = jnp.sum(jnp.where(small, jnp.broadcast_to(tw[...], (64, 64)), 0.0), axis=1, keepdims=True)
    for cp in qb:
        cp.wait_recv()
    tot = QB[0]
    for k in range(1, 16):
        tot = tot + QB[k]
    for r in range(2):
        for b in range(2):
            PK[b * 128 : b * 128 + 128, :] = to_col(tot[2 * r + b : 2 * r + b + 1, :])
        q = pr[r * 32 : r * 32 + 32, :]
        mass = jnp.sum(q, axis=1, keepdims=True)
        S["DV"][r * 32 : r * 32 + 32, :] = (
            jnp.sum(q * jnp.log(q), axis=1, keepdims=True) - PK[own, :] + mass * LN[r, own, :]
        )
    dv[...] = jnp.sum(jnp.where(small, jnp.broadcast_to(S["DV"][...], (64, 64)), 0.0), axis=0, keepdims=True)
    finish(0, p0, weight)
    finish(1, p1, weight)
    for cp in sent:
        cp.wait_send()


def hand_over(a, b, a_out, b_out, sem):
    copies = [pltpu.make_async_copy(a, a_out, sem.at[0]), pltpu.make_async_copy(b, b_out, sem.at[1])]
    for cp in copies:
        cp.start()
    for cp in copies:
        cp.wait()


def body(hidden, head_weight, teacher_ids, teacher_probs, token_weight):
    T, D = hidden.shape
    C = head_weight.shape[1]
    Z = D // 16
    V = pltpu.VMEM
    scratch = {
        "W": V((C, D), BF16), "H": V((2, 256, D), BF16), "IP": V((8, T, 128), F32),
        "SP": V((2, 256, C), F32), "L": V((2, 256, C), F32), "ST": V((256, 2), F32),
        "SA": V((2, 8, 8, 128), F32), "SB": V((2, 16, 8, 128), F32),
        "QA": V((8, 8, 128), F32), "QB": V((16, 8, 128), F32),
        "G": V((2, 256, C), BF16), "PK": V((256, 1), F32), "LN": V((2, 256, 1), F32),
        "DV": V((T, 1), F32),
        "PR": V((2, 16, 128, 256), F32), "DS": V((2, 16, 128, 256), BF16), "DR": V((2, 16, 128, 256), BF16),
        "ids": V(teacher_ids.shape, jnp.int32), "pr": V(teacher_probs.shape, F32), "tw": V((1, T), F32),
    }
    for r in range(2):
        for k, (_, tiles) in enumerate(COLOURS):
            n = len(tiles[r])
            scratch[f"T1{r}{k}"] = V((4, 16, n, 8, 128), BF16)
            scratch[f"R1{r}{k}"] = V((3, 16, n, 8, 128), BF16)
            scratch[f"T2{r}{k}"] = V((16, n, 8, 128), BF16)
            scratch[f"R2{r}{k}"] = V((15, n, 8, 128), BF16)
    scratch["ss"] = pltpu.SemaphoreType.DMA((260,))
    scratch["rs"] = pltpu.SemaphoreType.DMA((260,))
    scratch["hs"] = pltpu.SemaphoreType.REGULAR((3,))
    scratch["ls"] = pltpu.SemaphoreType.DMA((6,))
    vm = pl.BlockSpec(memory_space=pltpu.VMEM)
    grad, div = pl.pallas_call(
        functools.partial(kernel, names=tuple(scratch)),
        out_shape=(jax.ShapeDtypeStruct((T, Z), F32), jax.ShapeDtypeStruct((1, T), F32)),
        in_specs=[pl.BlockSpec(memory_space=pl.ANY)] * 5,
        out_specs=(vm, vm),
        scratch_shapes=list(scratch.values()),
        compiler_params=pltpu.CompilerParams(
            collective_id=0, has_side_effects=True, vmem_limit_bytes=67043328
        ),
        name="distill",
    )(hidden, head_weight.T, teacher_ids, teacher_probs, token_weight.reshape(1, T))
    grad, div = pl.pallas_call(
        hand_over,
        out_shape=(jax.ShapeDtypeStruct((T, Z), F32), jax.ShapeDtypeStruct((1, T), F32)),
        in_specs=[pl.BlockSpec(memory_space=pl.ANY)] * 2,
        out_specs=(pl.BlockSpec(memory_space=pl.ANY),) * 2,
        scratch_shapes=[pltpu.SemaphoreType.DMA((2,))],
        name="hand_over",
    )(grad, div)
    return div.reshape(T), grad


def solution(mesh):
    split = Mesh(mesh.devices.reshape(4, 2, 4, 4), ("x", "c", "y", "z"))
    placed = (P(DP, None), P(None, DP + VOCAB), P(DP, None), P(DP, None), P(DP))
    return jax.shard_map(
        body, mesh=split, in_specs=placed, out_specs=(P(DP), P(DP, VOCAB)), check_vma=False
    )
```
